32 devices in a mesh: sess: 16 (over z, x, core), exp: 2 (over y).
Axes of the slice: x: 2, y: 2, z: 4, core: 2. Of those that a mesh axis runs over, the one named last changes fastest.
Arguments:
- tokens: bfloat16 [16, 64, 4096], P('sess'), may hold values from -6 to 6
- routes: int32 [16, 64, 2], P('sess'), may hold values from 0 to 15, all different within a row; in each aligned block of 64 rows (0 to 63, 64 to 127, ..., all dimensions but the last counted through in order) at most 16 rows name the same one
- gates: float32 [16, 64, 2], P('sess'), may hold values from 0.2 to 1
- w_gate: bfloat16 [16, 4096, 1408], P('sess', None, 'exp'), may hold values from -0.09375 to 0.09375
- w_up: bfloat16 [16, 4096, 1408], P('sess', None, 'exp'), may hold values from -0.09375 to 0.09375
- w_down: bfloat16 [16, 1408, 4096], P('sess', 'exp'), may hold values from -0.15625 to 0.15625
- feat_gain: float32 [4096], replicated, may hold values from 0.25 to 1.75
- w_proj: bfloat16 [4096, 256], replicated, may hold values from -0.09375 to 0.09375
- conv_time: bfloat16 [3, 3, 3, 256, 256], replicated, may hold values from -0.078125 to 0.078125
- bias_time: float32 [256], replicated, may hold values from -3 to 3
- conv_space: bfloat16 [3, 3, 256, 256], replicated, may hold values from -0.125 to 0.125
- bias_space: float32 [256], replicated, may hold values from -3 to 3
- frame_cache: bfloat16 [3, 16, 16, 16, 256], P(None, 'sess', 'exp'), may hold values from -6 to 6
- cache_head: int32 [16], P('sess'), may hold values from 0 to 2
Outputs:
- out_frame: bfloat16 [16, 16, 16, 256], P('sess', 'exp')
The draws below stay inside these ranges and needn't reach their ends.
Inputs may be any that keep to these rules, and one draw needn't show every extreme that they name: `routes`: each token names 2 different experts; among the tokens of one session no expert is named more than 16 times, and in some sessions one is named exactly 16 times. The frame before the previous one is in slot (cache_head + 2) mod 3.
All inputs are finite; a program needn't handle non-finite values.
Results may differ from the reference program's by a relative error of at most 0.017.
Values may be sent and summed in bfloat16 or wider, within the bound.
A program may use at most 64 MiB of HBM per device.

```python
import math
import jax
import jax.numpy as jnp
import numpy as np
from jax import lax

D = 4096
HID = 1408
C = 256
TOPK = 2
GRID_W = 8
EXPERTS = 16
SESS = 16
GRID_H = 8
TOK_SESS = 64
CAP = 16
PH = 16
PW = 16
N_EXP = 2


def set_ends(drawn, key, low, largest):
    extent = drawn.shape
    place = [jax.random.randint(jax.random.fold_in(key, axis), (), 0, extent[axis]) for axis in range(len(extent))]
    drawn = drawn.at[tuple(place)].set(low)
    longest = extent.index(max(extent))
    place[longest] = (place[longest] + 1) % extent[longest]
    return drawn.at[tuple(place)].set(largest)


def block_levels(rng, extent, cuts, smallest, top_value):
    gain, own = 1.0, jax.random.fold_in(rng, 6)
    for dim, shards_of in cuts:
        draws = jnp.exp(jax.random.uniform(jax.random.fold_in(own, dim), (shards_of,), jnp.float32, smallest / len(cuts), top_value / len(cuts)))
        gain = gain * jnp.repeat(draws, extent[dim] // shards_of).reshape([-1 if axis == dim else 1 for axis in range(len(extent))])
    return gain


def shared_out(rng, own, number, rows, number_of, top, reach, slope):
    ranking = jax.random.permutation(rng, number_of)
    crowded, usual = portions_of(number_of, rows * top, reach, slope, True), portions_of(number_of, rows * top, reach, slope, False)
    places = jnp.arange(number_of)

    def named(lengths, turn):
        used = int((lengths > 0).sum())
        fixed = max(1, used // 4)
        shifted = fixed + (places - fixed + turn * (used - fixed)) % max(1, number_of - fixed)
        return jnp.zeros((number_of,), jnp.int32).at[ranking[jnp.where(places < fixed, places, shifted)]].set(jnp.asarray(lengths, jnp.int32))

    lengths = jnp.where(number % 4 == 0, named(crowded, number // 4), named(usual, number - number // 4 - 1))
    mixed = jax.random.permutation(jax.random.fold_in(own, 3), number_of)
    giver, sink = mixed[0:number_of // 2 * 2:2], mixed[1:number_of // 2 * 2:2]
    slack = jnp.minimum(lengths[giver] - 1, reach - lengths[sink]) // 2
    slack = jnp.where((giver == ranking[0]) | (sink == ranking[0]) | (lengths[sink] == 0), 0, jnp.maximum(slack, 0))
    shifted = jax.random.randint(jax.random.fold_in(own, 4), (number_of // 2,), 0, 1 << 20) % (slack + 1)
    lengths = lengths.at[giver].add(-shifted).at[sink].add(shifted)
    members = jnp.searchsorted(jnp.cumsum(lengths), jnp.arange(rows * top), side="right").astype(jnp.int32)
    table = members.reshape(top, rows).T
    table = table[jax.random.permutation(jax.random.fold_in(own, 1), rows)]
    turn = jax.random.randint(jax.random.fold_in(own, 2), (rows, 1), 0, top)
    return jnp.take_along_axis(table, (jnp.arange(top)[None, :] + turn) % top, axis=1)


def portions_of(number_of, total, limit, lean, full):
    weights = [(1 << 20) // math.isqrt(rank ** lean) + 1 for rank in range(1, number_of + 1)]
    largest = limit if full else min(limit, max(-(-total // number_of), total * weights[0] // sum(weights)))
    least = 1 if total - largest >= number_of - 1 else 0
    counts, spare = [largest] + [least] * (number_of - 1), total - largest - least * (number_of - 1)
    while spare > 0:
        movable = [i for i in range(1, number_of) if counts[i] < largest] or [i for i in range(1, number_of) if counts[i] < limit]
        whole, budget = sum([weights[i] for i in movable]), spare
        for i in movable:
            addition = min(limit - counts[i], max(1, budget * weights[i] // whole), spare)
            counts[i] = counts[i] + addition
            spare = spare - addition
    return np.array(counts)


def centred(rng, extent, scale, limit, cuts=(), kind=jnp.bfloat16):
    values = jax.random.normal(rng, extent, jnp.float32) * scale
    if len(cuts) > 0:
        values = block_levels(rng, extent, cuts, -0.22, 0.18) * values
    return jnp.clip(values, min=-limit, max=limit).astype(kind)


def setup_inputs(seed: int = 0) -> dict:
    keys = jax.random.split(jax.random.key(seed), 15)
    tokens = centred(keys[0], (SESS, TOK_SESS, D), 1.0, 6.0, ((0, 16),))
    routes_keys = jax.random.split(jax.random.fold_in(keys[1], 1), SESS * TOK_SESS // TOK_SESS)
    routes_turns = jax.random.permutation(jax.random.fold_in(keys[1], 3), SESS * TOK_SESS // TOK_SESS)
    routes = jax.vmap(lambda own, number: shared_out(jax.random.fold_in(keys[1], 2), own, number, TOK_SESS, EXPERTS, TOPK, CAP, 2))(routes_keys, routes_turns).reshape((SESS, TOK_SESS, TOPK))
    gates = jnp.clip(0.2 + 0.8 * jax.random.uniform(keys[2], (SESS, TOK_SESS, TOPK), jnp.float32) ** block_levels(keys[2], (SESS, TOK_SESS, TOPK), ((0, 16),), -0.2, 0.2), 0.2, 1.0)
    w_gate = centred(keys[3], (EXPERTS, D, HID), D ** -0.5, 0.09375, ((0, 16), (2, 2)))
    w_up = centred(keys[4], (EXPERTS, D, HID), D ** -0.5, 0.09375, ((0, 16), (2, 2)))
    w_down = centred(keys[5], (EXPERTS, HID, D), HID ** -0.5, 0.15625, ((0, 16), (1, 2)))
    feat_gain = jnp.clip(1.0 + 0.15 * jax.random.normal(keys[6], (D,), jnp.float32), 0.25, 1.75)
    w_proj = centred(keys[7], (D, C), D ** -0.5, 0.09375)
    conv_time = centred(keys[8], (3, 3, 3, C, C), (27 * C) ** -0.5, 0.078125)
    bias_time = centred(keys[9], (C,), 0.5, 3.0, (), jnp.float32)
    conv_space = centred(keys[10], (3, 3, C, C), (9 * C) ** -0.5, 0.125)
    bias_space = centred(keys[11], (C,), 0.5, 3.0, (), jnp.float32)
    frame_cache = centred(keys[12], (3, SESS, PH, PW, C), 1.0, 6.0, ((1, 16), (2, 2)))
    cache_head = set_ends(jax.random.randint(keys[13], (SESS,), 0, 3), jax.random.fold_in(keys[13], 1), 0, 2).astype(jnp.int32)
    return {"tokens": tokens, "routes": routes, "gates": gates, "w_gate": w_gate, "w_up": w_up, "w_down": w_down, "feat_gain": feat_gain, "w_proj": w_proj, "conv_time": conv_time, "bias_time": bias_time, "conv_space": conv_space, "bias_space": bias_space, "frame_cache": frame_cache, "cache_head": cache_head}


epsilon = 1e-06

def slot_targets(routes, experts, capacity):
    flat = routes.reshape(-1).astype(jnp.int32)
    onehot = (flat[:, None] == jnp.arange(experts, dtype=jnp.int32)[None, :]).astype(jnp.int32)
    before = jnp.cumsum(onehot, axis=0) - onehot
    position = lax.optimization_barrier(jnp.sum(before * onehot, axis=1))
    return (flat * capacity + position).astype(jnp.int32)

def pick_slot(cache, heads):
    choose = (jnp.arange(3, dtype=jnp.int32)[:, None] == heads[None, :]).astype(jnp.float32)
    return lax.optimization_barrier(jnp.sum(choose[:, :, None, None, None] * cache.astype(jnp.float32), axis=0)).astype(jnp.bfloat16)

def reference(tokens, routes, gates, w_gate, w_up, w_down, feat_gain, w_proj, conv_time, bias_time, conv_space, bias_space, frame_cache, cache_head):
    capacity = CAP
    slots = EXPERTS * capacity
    count = TOK_SESS * TOPK
    slice_width = HID // N_EXP
    dest = jax.vmap(lambda single: slot_targets(single, EXPERTS, capacity))(routes)
    filler = jnp.full((SESS, slots), count, jnp.int32)
    owner = jax.vmap(lambda base, target: base.at[target].set(jnp.arange(count, dtype=jnp.int32)))(filler, dest)
    padded = jnp.concatenate([tokens, jnp.zeros((SESS, 1, D), tokens.dtype)], axis=1)
    weights = jnp.concatenate([gates.reshape(SESS, count), jnp.zeros((SESS, 1), jnp.float32)], axis=1)
    session_ids = jnp.arange(SESS, dtype=jnp.int32)[:, None]

    def one_expert(total, expert):
        route_ids = lax.dynamic_slice_in_dim(owner, (expert * capacity).astype(jnp.int32), capacity, 1)
        token_ids = jnp.where(route_ids < count, route_ids // TOPK, TOK_SESS).astype(jnp.int32)
        rows = padded[session_ids, token_ids].reshape(SESS * capacity, D)
        gate = jnp.dot(rows, w_gate[expert], preferred_element_type=jnp.float32)
        upward = jnp.dot(rows, w_up[expert], preferred_element_type=jnp.float32)
        hidden = (jax.nn.silu(gate) * upward).astype(jnp.bfloat16)
        pieces = hidden.astype(jnp.float32).reshape(-1, N_EXP, slice_width)
        lowered = w_down[expert].astype(jnp.float32).reshape(N_EXP, slice_width, D)
        parts = jnp.einsum('rjh,jhd->rjd', pieces, lowered).astype(jnp.bfloat16)
        summed = lax.optimization_barrier(jnp.sum(parts.astype(jnp.float32), axis=1)).reshape(SESS, capacity, D)
        scale = weights[session_ids, route_ids]
        total = total.at[session_ids, token_ids].add(scale[:, :, None] * summed)
        return (total, None)
    start_total = jnp.zeros((SESS, TOK_SESS + 1, D), jnp.float32)
    total, _ = lax.scan(one_expert, start_total, jnp.arange(EXPERTS, dtype=jnp.int32))
    mixed = total[:, :TOK_SESS]
    feat = (tokens.astype(jnp.float32) + mixed).astype(jnp.bfloat16)
    square = lax.optimization_barrier(jnp.mean(jnp.square(feat.astype(jnp.float32)), axis=-1, keepdims=True))
    normed = (feat.astype(jnp.float32) * lax.rsqrt(square + epsilon) * feat_gain).astype(jnp.bfloat16)
    coarse = jnp.dot(normed.reshape(-1, D), w_proj, preferred_element_type=jnp.float32).astype(jnp.bfloat16)
    coarse = coarse.reshape(SESS, GRID_H, GRID_W, C)
    fine = jnp.repeat(jnp.repeat(coarse, 2, axis=1), 2, axis=2)
    latest = pick_slot(frame_cache, cache_head)
    older = pick_slot(frame_cache, (cache_head + 2) % 3)
    stack = jnp.stack([older, latest, fine])
    framed = jnp.pad(stack, ((0, 0), (0, 0), (1, 1), (1, 1), (0, 0)))
    first = jnp.zeros((SESS * PH * PW, C), jnp.float32)
    for frame_step in range(3):
        for row_step in range(3):
            for col_step in range(3):
                patch = framed[frame_step, :, row_step:row_step + PH, col_step:col_step + PW, :].reshape(-1, C)
                first = first + jnp.dot(patch, conv_time[frame_step, row_step, col_step], preferred_element_type=jnp.float32)
    active = jax.nn.silu(first + bias_time).astype(jnp.bfloat16).reshape(SESS, PH, PW, C)
    bordered = jnp.pad(active, ((0, 0), (1, 1), (1, 1), (0, 0)))
    second = jnp.zeros((SESS * PH * PW, C), jnp.float32)
    for row_step in range(3):
        for col_step in range(3):
            patch = bordered[:, row_step:row_step + PH, col_step:col_step + PW, :].reshape(-1, C)
            second = second + jnp.dot(patch, conv_space[row_step, col_step], preferred_element_type=jnp.float32)
    result = fine.astype(jnp.float32).reshape(-1, C) + second + bias_space
    return result.astype(jnp.bfloat16).reshape(SESS, PH, PW, C)
```

```python
import functools

import jax
import jax.numpy as jnp
from jax import lax
from jax.experimental import pallas as pl
from jax.experimental.pallas import tpu as pltpu
from jax.sharding import PartitionSpec as P

TOPK = 2
GRID_W = 8
HALO = 2
DIRECT = 4
MESH = pl.DeviceIdType.MESH
VMEM = pl.BlockSpec(memory_space=pltpu.VMEM)

epsilon = 1e-06


def partner(me, bits):
    other, weight = me, 1
    while bits:
        if bits & 1:
            other = other + weight * (1 - 2 * ((me // weight) % 2))
        bits //= 2
        weight *= 2
    return other


def silu(value):
    return value / (1.0 + jnp.exp(-value))


def across(left, right):
    return lax.dot_general(
        left, right, (((1,), (1,)), ((), ())), preferred_element_type=jnp.float32
    )


def pieces_of(part):
    unit = max(128, part // 8)
    sizes, left = [], part // unit
    while left > 0:
        take = 2 if left > 2 else 1
        sizes.append(take * unit)
        left -= take
    starts = [sum(sizes[:i]) for i in range(len(sizes))]
    return list(zip(starts, sizes))


def expert_kernel(
    sessions,
    tiles,
    cap,
    pieces,
    all_routes,
    all_gates,
    head,
    all_gain,
    all_tokens,
    w_gate,
    w_up,
    w_down,
    all_proj,
    all_cache,
    out,
    past,
    halo,
    routes,
    gates,
    gain,
    tokens,
    gate_w,
    up_w,
    down_w,
    w_proj,
    cache,
    near_hot,
    far_hot,
    near_mix,
    far_mix,
    hot_in,
    mix_in,
    relay_in,
    near_out,
    relay_out,
    rows_in,
    gate,
    upward,
    hidden,
    answer,
    stage,
    reduced,
    back,
    partial,
    summed,
    mine,
    theirs,
    load_sem,
    halo_sem,
    table_sem,
    token_sem,
    near_sem,
    far_sem,
    cross_sem,
    answer_sem,
    own_sem,
    other_sem,
    sum_sem,
    last_sem,
):
    me, tile = lax.axis_index("sess"), lax.axis_index("exp")
    half = sessions // 2
    direct = min(DIRECT, half)
    upper, h = me // half, me % half
    far = partner(me, half)
    span = half * cap
    part = rows_in.shape[2]
    width = part * tiles
    count, channels = tokens.shape[1], w_proj.shape[1]
    turns = range(len(pieces))

    def rows(index, base=0):
        return pl.ds(pl.multiple_of(base + index * cap, cap), cap)

    def peer(k):
        return partner(me, k), partner(h, k)

    def piece(j):
        begin, size = pieces[j]
        return slice(begin, begin + size)

    def remote(source, target, sems, where, device):
        return pltpu.make_async_remote_copy(
            src_ref=source,
            dst_ref=target,
            send_sem=sems.at[(0,) + where],
            recv_sem=sems.at[(1,) + where],
            device_id=device,
            device_id_type=MESH,
        )

    def drain(block, sems, where):
        pltpu.make_async_copy(block, block, sems.at[where]).wait()

    small = [
        pltpu.make_async_copy(all_routes, routes, load_sem.at[0]),
        pltpu.make_async_copy(all_gates, gates, load_sem.at[1]),
        pltpu.make_async_copy(all_cache, cache, load_sem.at[2]),
    ]
    token_loads = [
        pltpu.make_async_copy(
            all_tokens.at[:, m * part : (m + 1) * part], tokens.at[m], load_sem.at[3 + m]
        )
        for m in range(tiles)
    ]
    begin = pl.multiple_of(tile * part, part)
    big = [
        pltpu.make_async_copy(source, held, load_sem.at[3 + tiles + i])
        for i, (source, held) in enumerate(
            (
                (w_gate, gate_w),
                (w_up, up_w),
                (w_down, down_w),
                (all_proj.at[pl.ds(begin, part), :], w_proj),
                (all_gain.at[:, pl.ds(begin, part)], gain),
            )
        )
    ]
    for load in small + token_loads + big:
        load.start()

    barrier = pltpu.get_barrier_semaphore()
    for k in range(1, half + 1):
        pl.semaphore_signal(barrier, inc=1, device_id=(partner(me, k), tile), device_id_type=MESH)
    for m in range(1, tiles):
        pl.semaphore_signal(
            barrier, inc=1, device_id=(me, (tile + m) % tiles), device_id_type=MESH
        )

    small[0].wait()
    small[1].wait()
    expert = lax.broadcasted_iota(jnp.int32, (sessions, count), 0)
    named = [(routes[k : k + 1, :] == expert).astype(jnp.float32) for k in range(TOPK)]
    earlier = lax.broadcasted_iota(jnp.int32, (count, count), 0) < lax.broadcasted_iota(
        jnp.int32, (count, count), 1
    )
    before = jnp.dot(
        sum(named).astype(jnp.bfloat16),
        earlier.astype(jnp.float32).astype(jnp.bfloat16),
        preferred_element_type=jnp.float32,
    )
    targets = []
    for k in range(TOPK):
        place = jnp.sum(before * named[k], axis=0, keepdims=True).astype(jnp.int32)
        targets.append(routes[k : k + 1, :] * cap + place)
        before = before + named[k]
    for base, hot, mix in (
        (upper * span, near_hot, near_mix),
        ((1 - upper) * span, far_hot, far_mix),
    ):
        slot = base + lax.broadcasted_iota(jnp.int32, (span, count), 0)
        onehot = jnp.zeros((span, count), jnp.float32)
        weight = jnp.zeros((span, count), jnp.float32)
        for k in range(TOPK):
            hit = slot == targets[k]
            onehot = onehot + jnp.where(hit, 1.0, 0.0)
            weight = weight + jnp.where(hit, gates[k : k + 1, :], 0.0)
        weight = weight.T
        high = weight.astype(jnp.bfloat16)
        hot[...] = onehot.astype(jnp.bfloat16)
        mix[0] = high
        mix[1] = (weight - high.astype(jnp.float32)).astype(jnp.bfloat16)
    small[2].wait()
    chosen = head[0]
    frames = [cache[i] for i in range(3)]
    for t, shift in ((1, 0), (0, 2)):
        which = lax.rem(chosen + shift, 3)
        past[t] = jnp.where(which == 0, frames[0], jnp.where(which == 1, frames[1], frames[2]))
    for load in token_loads:
        load.wait()
    pl.semaphore_wait(barrier, half + tiles - 1)

    pending = [
        remote(far_hot, hot_in, table_sem, (0,), (far, tile)),
        remote(far_mix, mix_in, table_sem, (1,), (far, tile)),
    ]
    pending[0].start()
    near, relayed = {}, []
    for j in turns:
        here = piece(j)
        relayed.append(
            remote(
                tokens.at[tile, :, here], relay_in.at[:, here], token_sem, (j,), (far, tile)
            )
        )
        relayed[j].start()
        for m in range(tiles):
            near_out[m, :, here] = jnp.dot(
                near_hot[...], tokens[m, :, here], preferred_element_type=jnp.float32
            ).astype(jnp.bfloat16)
        for k in range(half - 1, 0, -1):
            other, index = peer(k)
            if k < direct:
                source, target = near_out.at[:, rows(index), here], rows_in.at[:, rows(h), here]
            else:
                source = near_out.at[tile, rows(index), here]
                target = rows_in.at[tile, rows(h), here]
            near[k, j] = remote(source, target, near_sem, (k, j), (other, tile))
            near[k, j].start()
        rows_in[:, rows(h), here] = near_out[:, rows(h), here]
    pending[1].start()
    height = past.shape[1]
    for side, first, step in ((0, height - HALO, 1), (1, 0, tiles - 1)):
        pending.append(
            remote(
                past.at[:, first : first + HALO],
                halo.at[side],
                halo_sem,
                (side,),
                (me, (tile + step) % tiles),
            )
        )
        pending[-1].start()
    pending[0].wait_recv()
    for load in big:
        load.wait()
    gate[...] = jnp.zeros_like(gate)
    upward[...] = jnp.zeros_like(upward)
    distant = {}

    def relay(j):
        here = piece(j)
        relayed[j].wait_recv()
        relay_out[:, here] = jnp.dot(
            hot_in[...], relay_in[:, here], preferred_element_type=jnp.float32
        ).astype(jnp.bfloat16)
        for k in range(half - 1, 0, -1):
            other, index = peer(k)
            distant[k, j] = remote(
                relay_out.at[rows(index), here],
                rows_in.at[tile, rows(h, span), here],
                far_sem,
                (k, j),
                (other, tile),
            )
            distant[k, j].start()
        rows_in[tile, rows(h, span), here] = relay_out[rows(h), here]

    def cross(j):
        here = piece(j)

        def forward(block):
            for m in range(1, tiles):
                remote(block, block, cross_sem, (m, j), (me, (tile + m) % tiles)).start()

        forward(rows_in.at[tile, rows(h, span), here])
        for k in range(direct, half):
            near[k, j].wait_recv()
            forward(rows_in.at[tile, rows(peer(k)[1]), here])
        for k in range(1, half):
            distant[k, j].wait_recv()
            forward(rows_in.at[tile, rows(peer(k)[1], span), here])

    def passed(j):
        return rows_in.at[0, pl.ds(0, (2 * half - direct) * cap), piece(j)]

    def consume(j):
        start, size = pieces[j]
        here = piece(j)
        for k in range(1, direct):
            near[k, j].wait_recv()
        for m in range(1, tiles):
            drain(passed(j), cross_sem, (1, m, j))

        @pl.loop(0, tiles)
        def _(m):
            span_in = pl.ds(pl.multiple_of(m * part + start, 128), size)
            block = rows_in[m, :, here]
            gate[...] += across(block, gate_w[:, span_in])
            upward[...] += across(block, up_w[:, span_in])

    for j in range(len(pieces) + 2):
        if j < len(pieces):
            relay(j)
        if 0 <= j - 1 < len(pieces):
            cross(j - 1)
        if 0 <= j - 2:
            consume(j - 2)
    hidden[...] = (silu(gate[...]) * upward[...]).astype(jnp.bfloat16)

    def project(m, j):
        start, size = pieces[j]
        span_in = pl.ds(pl.multiple_of(m * part + start, 128), size)
        return jnp.dot(hidden[...], down_w[:, span_in], preferred_element_type=jnp.float32)

    arrivals = {}
    for j in turns:
        here = piece(j)
        for m in range(1, tiles):
            to = (tile + m) % tiles
            answer[m - 1, :, here] = project(to, j).astype(jnp.bfloat16)
            arrivals[m, j] = remote(
                answer.at[m - 1, :, here], stage.at[m - 1, :, here], answer_sem, (m, j), (me, to)
            )
            arrivals[m, j].start()
    owns, others, sums = {}, {}, []

    def reduce(j):
        here = piece(j)
        total = project(tile, j)
        for m in range(1, tiles):
            arrivals[m, j].wait_recv()
            total = total + stage[m - 1, :, here].astype(jnp.float32)
        reduced[:, here] = total.astype(jnp.bfloat16)
        for k in range(half - 1, 0, -1):
            other, index = peer(k)
            for base, sems, made in ((span, other_sem, others), (0, own_sem, owns)):
                made[k, j] = remote(
                    reduced.at[rows(index, base), here],
                    back.at[rows(h, base), here],
                    sems,
                    (k, j),
                    (other, tile),
                )
                made[k, j].start()
        for base in (0, span):
            back[rows(h, base), here] = reduced[rows(h, base), here]

    def blend(mix, base, here):
        block = back[base : base + span, here]
        return jnp.dot(mix[0], block, preferred_element_type=jnp.float32) + jnp.dot(
            mix[1], block, preferred_element_type=jnp.float32
        )

    def give(j):
        here = piece(j)
        for k in range(1, half):
            others[k, j].wait_recv()
        if j == 0:
            pending[1].wait_recv()
        partial[:, here] = blend(mix_in, span, here).astype(jnp.bfloat16)
        sums.append(
            remote(partial.at[:, here], summed.at[:, here], sum_sem, (j,), (far, tile))
        )
        sums[j].start()

    square = jnp.zeros((count, 1), jnp.float32)
    coarse = jnp.zeros((count, channels), jnp.float32)
    for j in range(len(pieces) + 2):
        if j < len(pieces):
            reduce(j)
        if 0 <= j - 1 < len(pieces):
            give(j - 1)
        if 0 <= j - 2:
            here = piece(j - 2)
            for k in range(1, half):
                owns[k, j - 2].wait_recv()
            mixed = blend(near_mix, 0, here)
            sums[j - 2].wait_recv()
            mixed = mixed + summed[:, here].astype(jnp.float32)
            feat = (tokens[tile, :, here].astype(jnp.float32) + mixed).astype(jnp.bfloat16)
            feat = feat.astype(jnp.float32)
            square = square + jnp.sum(feat * feat, axis=1, keepdims=True)
            scaled = (feat * gain[:, here]).astype(jnp.bfloat16)
            coarse = coarse + jnp.dot(
                scaled, w_proj[here, :], preferred_element_type=jnp.float32
            )
    mine[:, :channels] = coarse
    mine[:, channels:] = jnp.broadcast_to(square, (count, 128))
    totals = []
    for m in range(1, tiles):
        totals.append(
            remote(mine, theirs.at[m - 1], last_sem, (m,), (me, (tile + m) % tiles))
        )
        totals[-1].start()
    for m, copy in enumerate(totals):
        copy.wait_recv()
        coarse = coarse + theirs[m, :, :channels]
        square = square + theirs[m, :, channels : channels + 1]
    out[...] = (coarse * lax.rsqrt(square * (1.0 / width) + epsilon)).astype(jnp.bfloat16).astype(
        jnp.float32
    )

    for copy in pending + relayed + sums + totals:
        copy.wait_send()
    for copy in pending[2:]:
        copy.wait_recv()
    for made in (near, distant, owns, others, arrivals):
        for copy in made.values():
            copy.wait_send()
    for j in turns:
        for m in range(1, tiles):
            drain(passed(j), cross_sem, (0, m, j))


def experts(routes, gates, head, gain, tokens, w_gate, w_up, w_down, w_proj, cache, sizes):
    sessions, tiles, cap = sizes
    count, width = tokens.shape
    hid, part, half = w_gate.shape[0], width // tiles, sessions // 2
    span, channels = half * cap, w_proj.shape[1]
    pieces = pieces_of(part)
    hbm = pl.BlockSpec(memory_space=pltpu.HBM)
    low, full = jnp.bfloat16, jnp.float32
    turns = len(pieces)
    return pl.pallas_call(
        functools.partial(expert_kernel, sessions, tiles, cap, pieces),
        out_shape=(
            jax.ShapeDtypeStruct((count, channels), full),
            jax.ShapeDtypeStruct((2,) + cache.shape[1:], cache.dtype),
            jax.ShapeDtypeStruct((2, 2, HALO) + cache.shape[2:], cache.dtype),
        ),
        in_specs=[hbm, hbm, pl.BlockSpec(memory_space=pltpu.SMEM)] + [hbm] * 7,
        out_specs=(VMEM,) * 3,
        scratch_shapes=[
            pltpu.VMEM(routes.shape, routes.dtype),
            pltpu.VMEM(gates.shape, gates.dtype),
            pltpu.VMEM((1, part), full),
            pltpu.VMEM((tiles, count, part), low),
            pltpu.VMEM((hid, width), low),
            pltpu.VMEM((hid, width), low),
            pltpu.VMEM((hid, width), low),
            pltpu.VMEM((part, channels), low),
            pltpu.VMEM(cache.shape, low),
            pltpu.VMEM((span, count), low),
            pltpu.VMEM((span, count), low),
            pltpu.VMEM((2, count, span), low),
            pltpu.VMEM((2, count, span), low),
            pltpu.VMEM((span, count), low),
            pltpu.VMEM((2, count, span), low),
            pltpu.VMEM((count, part), low),
            pltpu.VMEM((tiles, span, part), low),
            pltpu.VMEM((span, part), low),
            pltpu.VMEM((tiles, 2 * span, part), low),
            pltpu.VMEM((2 * span, hid), full),
            pltpu.VMEM((2 * span, hid), full),
            pltpu.VMEM((2 * span, hid), low),
            pltpu.VMEM((tiles - 1, 2 * span, part), low),
            pltpu.VMEM((tiles - 1, 2 * span, part), low),
            pltpu.VMEM((2 * span, part), low),
            pltpu.VMEM((2 * span, part), low),
            pltpu.VMEM((count, part), low),
            pltpu.VMEM((count, part), low),
            pltpu.VMEM((count, channels + 128), full),
            pltpu.VMEM((tiles - 1, count, channels + 128), full),
            pltpu.SemaphoreType.DMA((8 + tiles,)),
            pltpu.SemaphoreType.DMA((2, 2)),
            pltpu.SemaphoreType.DMA((2, 2)),
            pltpu.SemaphoreType.DMA((2, turns)),
            pltpu.SemaphoreType.DMA((2, half, turns)),
            pltpu.SemaphoreType.DMA((2, half, turns)),
            pltpu.SemaphoreType.DMA((2, tiles, turns)),
            pltpu.SemaphoreType.DMA((2, tiles, turns)),
            pltpu.SemaphoreType.DMA((2, half, turns)),
            pltpu.SemaphoreType.DMA((2, half, turns)),
            pltpu.SemaphoreType.DMA((2, turns)),
            pltpu.SemaphoreType.DMA((2, tiles)),
        ],
        compiler_params=pltpu.CompilerParams(
            collective_id=0, has_side_effects=True, vmem_limit_bytes=54 * 2**20
        ),
        name="experts",
    )(routes, gates, head, gain, tokens, w_gate, w_up, w_down, w_proj, cache)


def conv_kernel(
    coarse,
    past,
    halo,
    w_time,
    bias_time,
    w_space,
    bias_space,
    out,
    above,
    frames,
    wide,
    wide_active,
):
    tile, tiles = lax.axis_index("exp"), lax.axis_size("exp")
    tall, channels = frames.shape[1:]
    breadth = 2 * GRID_W
    edge = HALO * breadth
    count = out.shape[0]
    grid_rows = coarse.shape[0] // GRID_W
    own_rows = grid_rows // tiles

    for r in range(own_rows + 2):
        row = tile * own_rows - 1 + r
        at = jnp.clip(row, 0, grid_rows - 1)
        value = coarse[pl.ds(pl.multiple_of(at * GRID_W, GRID_W), GRID_W), :]
        above[r * GRID_W : (r + 1) * GRID_W, :] = jnp.where(
            (row >= 0) & (row < grid_rows), value, jnp.zeros_like(value)
        )
    for t in range(2):
        top, bottom = halo[0, t], halo[1, t]
        frames[t, :edge, :] = jnp.where(tile > 0, top, jnp.zeros_like(top))
        frames[t, edge : edge + count, :] = past[t]
        frames[t, edge + count :, :] = jnp.where(
            tile < tiles - 1, bottom, jnp.zeros_like(bottom)
        )

    def chosen(mask):
        return jnp.where(mask, 1.0, 0.0).astype(jnp.bfloat16)

    def moved(matrix, value):
        return jnp.dot(matrix, value, preferred_element_type=jnp.float32).astype(jnp.bfloat16)

    few = above.shape[0]
    pixel = lax.broadcasted_iota(jnp.int32, (tall, few), 0)
    token = lax.broadcasted_iota(jnp.int32, (tall, few), 1)
    spread = chosen(token == (pixel // (2 * breadth)) * GRID_W + (pixel % breadth) // 2)
    frames[2] = moved(spread, above[...].astype(jnp.bfloat16))

    def shifts(size):
        to = lax.broadcasted_iota(jnp.int32, (size, size), 0)
        origin = lax.broadcasted_iota(jnp.int32, (size, size), 1)
        column = to % breadth
        return (
            chosen((origin == to - 1) & (column > 0)),
            chosen((origin == to + 1) & (column < breadth - 1)),
        )

    left, right = shifts(tall)
    for t in range(3):
        wide[t, :, :channels] = moved(left, frames[t])
        wide[t, :, channels : 2 * channels] = frames[t]
        wide[t, :, 2 * channels :] = moved(right, frames[t])
    extended = count + 2 * breadth
    first = jnp.zeros((extended, channels), jnp.float32) + bias_time[...]
    for t in range(3):
        for dy in range(3):
            first = first + jnp.dot(
                wide[t, dy * breadth : dy * breadth + extended, :],
                w_time[3 * t + dy],
                preferred_element_type=jnp.float32,
            )
    row = tile * (count // breadth) - 1 + lax.broadcasted_iota(
        jnp.int32, (extended, channels), 0
    ) // breadth
    inside = (row >= 0) & (row < tiles * (count // breadth))
    active = jnp.where(inside, silu(first), 0.0).astype(jnp.bfloat16)
    left, right = shifts(extended)
    wide_active[:, :channels] = moved(left, active)
    wide_active[:, channels : 2 * channels] = active
    wide_active[:, 2 * channels :] = moved(right, active)
    total = frames[2, edge : edge + count, :].astype(jnp.float32) + bias_space[...]
    for dy in range(3):
        total = total + jnp.dot(
            wide_active[dy * breadth : dy * breadth + count, :],
            w_space[dy],
            preferred_element_type=jnp.float32,
        )
    out[...] = total.astype(jnp.bfloat16)


def decode(coarse, past, halo, w_time, bias_time, w_space, bias_space, tiles):
    count, channels = past.shape[1:]
    breadth = 2 * GRID_W
    tall = count + 2 * HALO * breadth
    few = coarse.shape[0] // tiles + 2 * GRID_W
    return pl.pallas_call(
        conv_kernel,
        out_shape=jax.ShapeDtypeStruct((count, channels), jnp.bfloat16),
        in_specs=[VMEM] * 7,
        out_specs=VMEM,
        scratch_shapes=[
            pltpu.VMEM((few, channels), jnp.float32),
            pltpu.VMEM((3, tall, channels), jnp.bfloat16),
            pltpu.VMEM((3, tall, 3 * channels), jnp.bfloat16),
            pltpu.VMEM((count + 2 * breadth, 3 * channels), jnp.bfloat16),
        ],
        compiler_params=pltpu.CompilerParams(vmem_limit_bytes=24 * 2**20),
        name="decode",
    )(coarse, past, halo, w_time, bias_time, w_space, bias_space)


def body(
    tokens,
    routes,
    gates,
    w_gate,
    w_up,
    w_down,
    feat_gain,
    w_proj,
    conv_time,
    bias_time,
    conv_space,
    bias_space,
    frame_cache,
    cache_head,
):
    sessions, tiles = lax.axis_size("sess"), lax.axis_size("exp")
    channels = w_proj.shape[-1]
    local = tokens[0]
    tok_count = local.shape[0]
    cap = 2 * tok_count * TOPK // sessions
    height, breadth = frame_cache.shape[2:4]
    coarse, past, halo = experts(
        routes[0].T,
        gates[0].T,
        cache_head,
        feat_gain[None, :],
        local,
        w_gate[0].T,
        w_up[0].T,
        w_down[0],
        w_proj,
        frame_cache[:, 0],
        (sessions, tiles, cap),
    )
    result = decode(
        coarse,
        past.reshape(2, height * breadth, channels),
        halo.reshape(2, 2, HALO * breadth, channels),
        conv_time.reshape(9, 3 * channels, channels),
        bias_time[None, :],
        conv_space.reshape(3, 3 * channels, channels),
        bias_space[None, :],
        tiles,
    )
    return result.reshape(1, height, breadth, channels)


def solution(mesh):
    return jax.shard_map(
        body,
        mesh=mesh,
        in_specs=(
            P("sess", None, None),
            P("sess", None, None),
            P("sess", None, None),
            P("sess", None, "exp"),
            P("sess", None, "exp"),
            P("sess", "exp", None),
            P(),
            P(),
            P(),
            P(),
            P(),
            P(),
            P(None, "sess", "exp", None, None),
            P("sess"),
        ),
        out_specs=P("sess", "exp", None, None),
        check_vma=False,
    )
```

```python
import functools

import jax
import jax.numpy as jnp
from jax import lax
from jax.experimental import pallas as pl
from jax.experimental.pallas import tpu as pltpu
from jax.sharding import PartitionSpec as P

TOPK = 2
GRID_W = 8
HALO = 2
DIRECT = 4
MESH = pl.DeviceIdType.MESH
VMEM = pl.BlockSpec(memory_space=pltpu.VMEM)

epsilon = 1e-06


def partner(me, bits):
    other, weight = me, 1
    while bits:
        if bits & 1:
            other = other + weight * (1 - 2 * ((me // weight) % 2))
        bits //= 2
        weight *= 2
    return other


def silu(value):
    return value / (1.0 + jnp.exp(-value))


def across(left, right):
    return lax.dot_general(
        left, right, (((1,), (1,)), ((), ())), preferred_element_type=jnp.float32
    )


def pieces_of(part):
    unit = max(128, part // 8)
    sizes, left = [], part // unit
    while left > 0:
        take = 2 if left > 2 else 1
        sizes.append(take * unit)
        left -= take
    starts = [sum(sizes[:i]) for i in range(len(sizes))]
    return list(zip(starts, sizes))


def layer_kernel(
    sessions,
    tiles,
    cap,
    pieces,
    all_routes,
    all_gates,
    head,
    all_gain,
    all_tokens,
    w_gate,
    w_up,
    w_down,
    all_proj,
    all_cache,
    all_time,
    all_time_bias,
    all_space,
    all_space_bias,
    out,
    routes,
    gates,
    gain,
    tokens,
    gate_w,
    up_w,
    down_w,
    w_proj,
    cache,
    w_time,
    bias_time,
    w_space,
    bias_space,
    past,
    halo,
    near_hot,
    far_hot,
    near_mix,
    far_mix,
    hot_in,
    mix_in,
    relay_in,
    near_out,
    relay_out,
    rows_in,
    gate,
    upward,
    hidden,
    near_answer,
    near_back,
    near_mixed,
    own_mixed,
    mixed_in,
    answer,
    stage,
    reduced,
    back,
    partial,
    summed,
    mine,
    theirs,
    coarse_in,
    above,
    frames,
    wide,
    first,
    wide_active,
    load_sem,
    halo_sem,
    table_sem,
    token_sem,
    near_sem,
    far_sem,
    near_cross,
    far_cross,
    back_sem,
    mixed_sem,
    answer_sem,
    other_sem,
    sum_sem,
    last_sem,
):
    me, tile = lax.axis_index("sess"), lax.axis_index("exp")
    half = sessions // 2
    direct = min(DIRECT, half)
    upper, h = me // half, me % half
    far = partner(me, half)
    span = half * cap
    part = rows_in.shape[2]
    width = part * tiles
    count, channels = tokens.shape[1], w_proj.shape[1]
    turns = range(len(pieces))

    def rows(index, base=0):
        return pl.ds(pl.multiple_of(base + index * cap, cap), cap)

    def peer(k):
        return partner(me, k), partner(h, k)

    def piece(j):
        begin, size = pieces[j]
        return slice(begin, begin + size)

    def columns(m, j):
        begin, size = pieces[j]
        return pl.ds(pl.multiple_of(m * part + begin, 128), size)

    def remote(source, target, sems, where, device):
        return pltpu.make_async_remote_copy(
            src_ref=source,
            dst_ref=target,
            send_sem=sems.at[(0,) + where],
            recv_sem=sems.at[(1,) + where],
            device_id=device,
            device_id_type=MESH,
        )

    def drain(block, sems, where):
        pltpu.make_async_copy(block, block, sems.at[where]).wait()

    begin = pl.multiple_of(tile * part, part)
    sources = [(all_routes, routes), (all_gates, gates)]
    sources += [
        (all_tokens.at[:, m * part : (m + 1) * part], tokens.at[m]) for m in range(tiles)
    ]
    sources += [
        (all_cache, cache),
        (w_gate, gate_w),
        (w_up, up_w),
        (w_down, down_w),
        (all_time, w_time),
        (all_time_bias, bias_time),
        (all_space, w_space),
        (all_space_bias, bias_space),
        (all_proj.at[pl.ds(begin, part), :], w_proj),
        (all_gain.at[:, pl.ds(begin, part)], gain),
    ]
    loads = [
        pltpu.make_async_copy(source, held, load_sem.at[i])
        for i, (source, held) in enumerate(sources)
    ]
    for load in loads:
        load.start()
    token_loads, loads = loads[: 2 + tiles], loads[2 + tiles :]

    barrier = pltpu.get_barrier_semaphore()
    for k in range(1, half + 1):
        pl.semaphore_signal(barrier, inc=1, device_id=(partner(me, k), tile), device_id_type=MESH)
    for m in range(1, tiles):
        pl.semaphore_signal(
            barrier, inc=1, device_id=(me, (tile + m) % tiles), device_id_type=MESH
        )

    token_loads[0].wait()
    token_loads[1].wait()
    expert = lax.broadcasted_iota(jnp.int32, (sessions, count), 0)
    named = [(routes[k : k + 1, :] == expert).astype(jnp.float32) for k in range(TOPK)]
    earlier = lax.broadcasted_iota(jnp.int32, (count, count), 0) < lax.broadcasted_iota(
        jnp.int32, (count, count), 1
    )
    before = jnp.dot(
        sum(named).astype(jnp.bfloat16),
        earlier.astype(jnp.float32).astype(jnp.bfloat16),
        preferred_element_type=jnp.float32,
    )
    targets = []
    for k in range(TOPK):
        place = jnp.sum(before * named[k], axis=0, keepdims=True).astype(jnp.int32)
        targets.append(routes[k : k + 1, :] * cap + place)
        before = before + named[k]
    weights = []
    for base, hot in ((upper * span, near_hot), ((1 - upper) * span, far_hot)):
        slot = base + lax.broadcasted_iota(jnp.int32, (span, count), 0)
        onehot = jnp.zeros((span, count), jnp.float32)
        weight = jnp.zeros((span, count), jnp.float32)
        for k in range(TOPK):
            hit = slot == targets[k]
            onehot = onehot + jnp.where(hit, 1.0, 0.0)
            weight = weight + jnp.where(hit, gates[k : k + 1, :], 0.0)
        hot[...] = onehot.astype(jnp.bfloat16)
        weights.append(weight)
    for load in token_loads[2:]:
        load.wait()
    pl.semaphore_wait(barrier, half + tiles - 1)

    pending = [remote(far_hot, hot_in, table_sem, (0,), (far, tile))]
    pending[0].start()
    relayed = [
        remote(
            tokens.at[tile, :, piece(j)], relay_in.at[:, piece(j)], token_sem, (j,), (far, tile)
        )
        for j in turns
    ]
    relayed[0].start()
    near = {}
    for j in turns:
        here = piece(j)
        for m in range(tiles):
            near_out[m, :, here] = jnp.dot(
                near_hot[...], tokens[m, :, here], preferred_element_type=jnp.float32
            ).astype(jnp.bfloat16)
        for k in range(half - 1, 0, -1):
            other, index = peer(k)
            if k < direct:
                source, target = near_out.at[:, rows(index), here], rows_in.at[:, rows(h), here]
            else:
                source = near_out.at[tile, rows(index), here]
                target = rows_in.at[tile, rows(h), here]
            near[k, j] = remote(source, target, near_sem, (k, j), (other, tile))
            near[k, j].start()
        rows_in[:, rows(h), here] = near_out[:, rows(h), here]
    for copy in relayed[1:]:
        copy.start()
    for weight, mix in zip(weights, (near_mix, far_mix)):
        weight = weight.T
        high = weight.astype(jnp.bfloat16)
        mix[0] = high
        mix[1] = (weight - high.astype(jnp.float32)).astype(jnp.bfloat16)
    pending.append(remote(far_mix, mix_in, table_sem, (1,), (far, tile)))
    pending[1].start()

    loads[0].wait()
    newest = head[0]
    slots = [cache[i] for i in range(3)]
    for t, shift in ((1, 0), (0, 2)):
        which = lax.rem(newest + shift, 3)
        past[t] = jnp.where(which == 0, slots[0], jnp.where(which == 1, slots[1], slots[2]))
    height = past.shape[1]
    for side, start, step in ((0, height - HALO, 1), (1, 0, tiles - 1)):
        pending.append(
            remote(
                past.at[:, start : start + HALO],
                halo.at[side],
                halo_sem,
                (side,),
                (me, (tile + step) % tiles),
            )
        )
        pending[-1].start()

    distant = {}

    def forward(block, sems, j):
        for m in range(1, tiles):
            remote(block, block, sems, (m, j), (me, (tile + m) % tiles)).start()

    def near_forward(j):
        for k in range(direct, half):
            near[k, j].wait_recv()
            forward(rows_in.at[tile, rows(peer(k)[1]), piece(j)], near_cross, j)

    def relay(j):
        here = piece(j)
        if j == 0:
            pending[0].wait_recv()
        relayed[j].wait_recv()
        relay_out[:, here] = jnp.dot(
            hot_in[...], relay_in[:, here], preferred_element_type=jnp.float32
        ).astype(jnp.bfloat16)
        for k in range(half - 1, 0, -1):
            other, index = peer(k)
            distant[k, j] = remote(
                relay_out.at[rows(index), here],
                rows_in.at[tile, rows(h, span), here],
                far_sem,
                (k, j),
                (other, tile),
            )
            distant[k, j].start()
        rows_in[tile, rows(h, span), here] = relay_out[rows(h), here]

    def far_forward(j):
        here = piece(j)
        forward(rows_in.at[tile, rows(h, span), here], far_cross, j)
        for k in range(1, half):
            distant[k, j].wait_recv()
            forward(rows_in.at[tile, rows(peer(k)[1], span), here], far_cross, j)

    def near_passed(j):
        return rows_in.at[0, pl.ds(0, (half - direct) * cap), piece(j)]

    def far_passed(j):
        return rows_in.at[0, pl.ds(0, span), piece(j)]

    def consume(group, j):
        base = group * span
        if group == 0:
            for k in range(1, direct):
                near[k, j].wait_recv()
        for m in range(1, tiles):
            if group == 0:
                drain(near_passed(j), near_cross, (1, m, j))
            else:
                drain(far_passed(j), far_cross, (1, m, j))
        if j == 0:
            gate[...] = jnp.zeros_like(gate)
            upward[...] = jnp.zeros_like(upward)

        @pl.loop(0, tiles)
        def _(m):
            block = rows_in[m, base : base + span, piece(j)]
            gate[...] += across(block, gate_w[:, columns(m, j)])
            upward[...] += across(block, up_w[:, columns(m, j)])

    def activate(group):
        hidden[group] = (silu(gate[...]) * upward[...]).astype(jnp.bfloat16)

    def project(group, m, j):
        return jnp.dot(
            hidden[group], down_w[:, columns(m, j)], preferred_element_type=jnp.float32
        )

    home, tied = {}, {}

    def near_return(j):
        here = piece(j)

        @pl.loop(0, tiles)
        def _(m):
            near_answer[m, :, here] = project(0, m, j).astype(jnp.bfloat16)

        for k in range(half - 1, 0, -1):
            other, index = peer(k)
            home[k, j] = remote(
                near_answer.at[:, rows(index), here],
                near_back.at[:, rows(h), here],
                back_sem,
                (k, j),
                (other, tile),
            )
            home[k, j].start()
        near_back[:, rows(h), here] = near_answer[:, rows(h), here]

    def blend(mix, block):
        return jnp.dot(mix[0], block, preferred_element_type=jnp.float32) + jnp.dot(
            mix[1], block, preferred_element_type=jnp.float32
        )

    def near_blend(j):
        here = piece(j)
        for k in range(1, half):
            home[k, j].wait_recv()
        for m in range(1, tiles):
            to = (tile + m) % tiles
            near_mixed[m - 1, :, here] = blend(near_mix, near_back[to, :, here]).astype(
                jnp.bfloat16
            )
            tied[m, j] = remote(
                near_mixed.at[m - 1, :, here],
                mixed_in.at[m - 1, :, here],
                mixed_sem,
                (m, j),
                (me, to),
            )
            tied[m, j].start()
        own_mixed[:, here] = blend(near_mix, near_back[tile, :, here])

    arrivals, others, sums = {}, {}, []

    def far_answer(j):
        here = piece(j)
        for m in range(1, tiles):
            to = (tile + m) % tiles
            answer[m - 1, :, here] = project(1, to, j).astype(jnp.bfloat16)
            arrivals[m, j] = remote(
                answer.at[m - 1, :, here], stage.at[m - 1, :, here], answer_sem, (m, j), (me, to)
            )
            arrivals[m, j].start()

    def far_return(j):
        here = piece(j)
        total = project(1, tile, j)
        for m in range(1, tiles):
            arrivals[m, j].wait_recv()
            total = total + stage[m - 1, :, here].astype(jnp.float32)
        reduced[:, here] = total.astype(jnp.bfloat16)
        for k in range(half - 1, 0, -1):
            other, index = peer(k)
            others[k, j] = remote(
                reduced.at[rows(index), here],
                back.at[rows(h), here],
                other_sem,
                (k, j),
                (other, tile),
            )
            others[k, j].start()
        back[rows(h), here] = reduced[rows(h), here]

    def far_blend(j):
        here = piece(j)
        if j == 0:
            pending[1].wait_recv()
        for k in range(1, half):
            others[k, j].wait_recv()
        partial[:, here] = blend(mix_in, back[:, here]).astype(jnp.bfloat16)
        sums.append(
            remote(partial.at[:, here], summed.at[:, here], sum_sem, (j,), (far, tile))
        )
        sums[j].start()

    def features(j):
        here = piece(j)
        mixed = own_mixed[:, here]
        for m in range(1, tiles):
            tied[m, j].wait_recv()
            mixed = mixed + mixed_in[m - 1, :, here].astype(jnp.float32)
        sums[j].wait_recv()
        mixed = mixed + summed[:, here].astype(jnp.float32)
        feat = (tokens[tile, :, here].astype(jnp.float32) + mixed).astype(jnp.bfloat16)
        feat = feat.astype(jnp.float32)
        scaled = (feat * gain[:, here]).astype(jnp.bfloat16)
        return (
            jnp.sum(feat * feat, axis=1, keepdims=True),
            jnp.dot(scaled, w_proj[here, :], preferred_element_type=jnp.float32),
        )

    tall = frames.shape[1]
    breadth = 2 * GRID_W
    edge = HALO * breadth
    pixels = out.shape[0]
    extended = pixels + 2 * breadth
    grid_rows = count // GRID_W
    own_rows = grid_rows // tiles

    def chosen(mask):
        return jnp.where(mask, 1.0, 0.0).astype(jnp.bfloat16)

    def moved(matrix, value):
        return jnp.dot(matrix, value, preferred_element_type=jnp.float32).astype(jnp.bfloat16)

    def shifts(size):
        to = lax.broadcasted_iota(jnp.int32, (size, size), 0)
        origin = lax.broadcasted_iota(jnp.int32, (size, size), 1)
        column = to % breadth
        return (
            chosen((origin == to - 1) & (column > 0)),
            chosen((origin == to + 1) & (column < breadth - 1)),
        )

    def widen(t, left, right):
        wide[t, :, :channels] = moved(left, frames[t])
        wide[t, :, channels : 2 * channels] = frames[t]
        wide[t, :, 2 * channels :] = moved(right, frames[t])

    def in_time(t):
        total = jnp.zeros((extended, channels), jnp.float32)
        for dy in range(3):
            total = total + jnp.dot(
                wide[t, dy * breadth : dy * breadth + extended, :],
                w_time[3 * t + dy],
                preferred_element_type=jnp.float32,
            )
        return total

    def earlier_frames():
        for copy in pending[2:]:
            copy.wait_recv()
        left, right = shifts(tall)
        for t in range(2):
            top = halo[0, t].reshape(edge, channels)
            bottom = halo[1, t].reshape(edge, channels)
            frames[t, :edge, :] = jnp.where(tile > 0, top, jnp.zeros_like(top))
            frames[t, edge : edge + pixels, :] = past[t].reshape(pixels, channels)
            frames[t, edge + pixels :, :] = jnp.where(
                tile < tiles - 1, bottom, jnp.zeros_like(bottom)
            )
            widen(t, left, right)
        first[...] = in_time(0) + in_time(1) + bias_time[...]

    def last_frame():
        for r in range(own_rows + 2):
            row = tile * own_rows - 1 + r
            at = jnp.clip(row, 0, grid_rows - 1)
            value = coarse_in[pl.ds(pl.multiple_of(at * GRID_W, GRID_W), GRID_W), :]
            above[r * GRID_W : (r + 1) * GRID_W, :] = jnp.where(
                (row >= 0) & (row < grid_rows), value, jnp.zeros_like(value)
            )
        few = above.shape[0]
        pixel = lax.broadcasted_iota(jnp.int32, (tall, few), 0)
        token = lax.broadcasted_iota(jnp.int32, (tall, few), 1)
        spread = chosen(token == (pixel // (2 * breadth)) * GRID_W + (pixel % breadth) // 2)
        frames[2] = moved(spread, above[...].astype(jnp.bfloat16))
        left, right = shifts(tall)
        widen(2, left, right)
        total = first[...] + in_time(2)
        row = tile * (pixels // breadth) - 1 + lax.broadcasted_iota(
            jnp.int32, (extended, channels), 0
        ) // breadth
        inside = (row >= 0) & (row < tiles * (pixels // breadth))
        active = jnp.where(inside, silu(total), 0.0).astype(jnp.bfloat16)
        left, right = shifts(extended)
        wide_active[:, :channels] = moved(left, active)
        wide_active[:, channels : 2 * channels] = active
        wide_active[:, 2 * channels :] = moved(right, active)
        total = frames[2, edge : edge + pixels, :].astype(jnp.float32) + bias_space[...]
        for dy in range(3):
            total = total + jnp.dot(
                wide_active[dy * breadth : dy * breadth + pixels, :],
                w_space[dy],
                preferred_element_type=jnp.float32,
            )
        out[...] = total.astype(jnp.bfloat16)

    n = len(pieces)

    def steps(*stages):
        reach = n + max(lag for lag, _ in stages)
        for j in range(reach):
            for lag, stage_of in stages:
                if 0 <= j - lag < n:
                    stage_of(j - lag)

    for load in loads[1:3]:
        load.wait()
    steps((0, near_forward), (1, functools.partial(consume, 0)))
    activate(0)
    steps((0, relay), (3, far_forward))
    loads[3].wait()
    steps((0, near_return), (1, functools.partial(consume, 1)))
    activate(1)
    steps((0, far_answer))
    steps((0, near_blend))
    for load in loads[4:]:
        load.wait()
    earlier_frames()
    found = []
    steps((0, far_return), (1, far_blend), (2, lambda j: found.append(features(j))))
    square = sum(pair[0] for pair in found)
    coarse = sum(pair[1] for pair in found)
    lane = lax.broadcasted_iota(jnp.int32, (count, 128), 1)
    high = square.astype(jnp.bfloat16).astype(jnp.float32)
    mine[:, :channels] = coarse.astype(jnp.bfloat16)
    mine[:, channels:] = jnp.where(
        lane == 0, high, jnp.where(lane == 1, square - high, 0.0)
    ).astype(jnp.bfloat16)
    totals = []
    for m in range(1, tiles):
        totals.append(
            remote(mine, theirs.at[m - 1], last_sem, (m,), (me, (tile + m) % tiles))
        )
        totals[-1].start()
    for m, copy in enumerate(totals):
        copy.wait_recv()
        coarse = coarse + theirs[m, :, :channels].astype(jnp.float32)
        square = square + jnp.sum(
            theirs[m, :, channels:].astype(jnp.float32), axis=1, keepdims=True
        )
    coarse_in[...] = coarse * lax.rsqrt(square * (1.0 / width) + epsilon)
    last_frame()

    for copy in pending + relayed + sums + totals:
        copy.wait_send()
    for made in (near, distant, home, tied, others, arrivals):
        for copy in made.values():
            copy.wait_send()
    for j in turns:
        for m in range(1, tiles):
            drain(near_passed(j), near_cross, (0, m, j))
            drain(far_passed(j), far_cross, (0, m, j))


def layer(
    routes,
    gates,
    head,
    gain,
    tokens,
    w_gate,
    w_up,
    w_down,
    w_proj,
    cache,
    w_time,
    bias_time,
    w_space,
    bias_space,
    sizes,
):
    sessions, tiles, cap = sizes
    count, width = tokens.shape
    hid, part, half = w_gate.shape[0], width // tiles, sessions // 2
    span, channels = half * cap, w_proj.shape[1]
    pixels = cache.shape[1] * cache.shape[2]
    breadth = 2 * GRID_W
    tall = pixels + 2 * HALO * breadth
    few = count // tiles + 2 * GRID_W
    pieces = pieces_of(part)
    hbm = pl.BlockSpec(memory_space=pltpu.HBM)
    low, full = jnp.bfloat16, jnp.float32
    n = len(pieces)
    held = [
        (routes.shape, routes.dtype),
        (gates.shape, full),
        ((1, part), full),
        ((tiles, count, part), low),
        (w_gate.shape, low),
        (w_up.shape, low),
        (w_down.shape, low),
        ((part, channels), low),
        (cache.shape, low),
        (w_time.shape, low),
        (bias_time.shape, full),
        (w_space.shape, low),
        (bias_space.shape, full),
        ((2,) + cache.shape[1:], low),
        ((2, 2, HALO) + cache.shape[2:], low),
        ((span, count), low),
        ((span, count), low),
        ((2, count, span), low),
        ((2, count, span), low),
        ((span, count), low),
        ((2, count, span), low),
        ((count, part), low),
        ((tiles, span, part), low),
        ((span, part), low),
        ((tiles, 2 * span, part), low),
        ((span, hid), full),
        ((span, hid), full),
        ((2, span, hid), low),
        ((tiles, span, part), low),
        ((tiles, span, part), low),
        ((tiles - 1, count, part), low),
        ((count, part), full),
        ((tiles - 1, count, part), low),
        ((tiles - 1, span, part), low),
        ((tiles - 1, span, part), low),
        ((span, part), low),
        ((span, part), low),
        ((count, part), low),
        ((count, part), low),
        ((count, channels + 128), low),
        ((tiles - 1, count, channels + 128), low),
        ((count, channels), full),
        ((few, channels), full),
        ((3, tall, channels), low),
        ((3, tall, 3 * channels), low),
        ((pixels + 2 * breadth, channels), full),
        ((pixels + 2 * breadth, 3 * channels), low),
    ]
    sems = [
        (12 + tiles,),
        (2, 2),
        (2, 2),
        (2, n),
        (2, half, n),
        (2, half, n),
        (2, tiles, n),
        (2, tiles, n),
        (2, half, n),
        (2, tiles, n),
        (2, tiles, n),
        (2, half, n),
        (2, n),
        (2, tiles),
    ]
    return pl.pallas_call(
        functools.partial(layer_kernel, sessions, tiles, cap, pieces),
        out_shape=jax.ShapeDtypeStruct((pixels, channels), low),
        in_specs=[hbm, hbm, pl.BlockSpec(memory_space=pltpu.SMEM)] + [hbm] * 11,
        out_specs=VMEM,
        scratch_shapes=[pltpu.VMEM(*each) for each in held]
        + [pltpu.SemaphoreType.DMA(each) for each in sems],
        compiler_params=pltpu.CompilerParams(
            collective_id=0, has_side_effects=True, vmem_limit_bytes=60 * 2**20
        ),
        name="layer",
    )(
        routes,
        gates,
        head,
        gain,
        tokens,
        w_gate,
        w_up,
        w_down,
        w_proj,
        cache,
        w_time,
        bias_time,
        w_space,
        bias_space,
    )


def body(
    tokens,
    routes,
    gates,
    w_gate,
    w_up,
    w_down,
    feat_gain,
    w_proj,
    conv_time,
    bias_time,
    conv_space,
    bias_space,
    frame_cache,
    cache_head,
):
    sessions, tiles = lax.axis_size("sess"), lax.axis_size("exp")
    channels = w_proj.shape[-1]
    local = tokens[0]
    tok_count = local.shape[0]
    cap = 2 * tok_count * TOPK // sessions
    height, breadth = frame_cache.shape[2:4]
    result = layer(
        routes[0].T,
        gates[0].T,
        cache_head,
        feat_gain[None, :],
        local,
        w_gate[0].T,
        w_up[0].T,
        w_down[0],
        w_proj,
        frame_cache[:, 0],
        conv_time.reshape(9, 3 * channels, channels),
        bias_time[None, :],
        conv_space.reshape(3, 3 * channels, channels),
        bias_space[None, :],
        (sessions, tiles, cap),
    )
    return result.reshape(1, height, breadth, channels)


def solution(mesh):
    return jax.shard_map(
        body,
        mesh=mesh,
        in_specs=(
            P("sess", None, None),
            P("sess", None, None),
            P("sess", None, None),
            P("sess", None, "exp"),
            P("sess", None, "exp"),
            P("sess", "exp", None),
            P(),
            P(),
            P(),
            P(),
            P(),
            P(),
            P(None, "sess", "exp", None, None),
            P("sess"),
        ),
        out_specs=P("sess", "exp", None, None),
        check_vma=False,
    )
```

```python
import functools

import jax
import jax.numpy as jnp
from jax import lax
from jax.experimental import pallas as pl
from jax.experimental.pallas import tpu as pltpu
from jax.sharding import PartitionSpec as P

TOPK = 2
GRID_W = 8
HALO = 2
DIRECT = 4
MESH = pl.DeviceIdType.MESH
VMEM = pl.BlockSpec(memory_space=pltpu.VMEM)

epsilon = 1e-06


def partner(me, bits):
    other, weight = me, 1
    while bits:
        if bits & 1:
            other = other + weight * (1 - 2 * ((me // weight) % 2))
        bits //= 2
        weight *= 2
    return other


def silu(value):
    return value / (1.0 + jnp.exp(-value))


def across(left, right):
    return lax.dot_general(
        left, right, (((1,), (1,)), ((), ())), preferred_element_type=jnp.float32
    )


def pieces_of(part):
    size = max(128, part // 4)
    return [(begin, size) for begin in range(0, part, size)]


def layer_kernel(
    sessions,
    tiles,
    cap,
    pieces,
    all_routes,
    all_gates,
    head,
    all_gain,
    all_tokens,
    w_gate,
    w_up,
    w_down,
    all_proj,
    all_cache,
    all_time,
    all_time_bias,
    all_space,
    all_space_bias,
    out,
    routes,
    gates,
    gain,
    tokens,
    gate_w,
    up_w,
    down_w,
    w_proj,
    cache,
    w_time,
    bias_time,
    w_space,
    bias_space,
    past,
    halo,
    near_hot,
    far_hot,
    near_mix,
    far_mix,
    hot_in,
    mix_in,
    relay_in,
    near_out,
    relay_out,
    rows_in,
    gate,
    upward,
    hidden,
    near_answer,
    near_back,
    near_mixed,
    own_mixed,
    mixed_in,
    answer,
    stage,
    reduced,
    back,
    partial,
    summed,
    mine,
    theirs,
    coarse_in,
    above,
    frames,
    wide,
    first,
    wide_active,
    load_sem,
    halo_sem,
    table_sem,
    token_sem,
    near_sem,
    direct_sem,
    far_sem,
    near_cross,
    far_cross,
    back_sem,
    mixed_sem,
    answer_sem,
    other_sem,
    sum_sem,
    last_sem,
):
    me, tile = lax.axis_index("sess"), lax.axis_index("exp")
    half = sessions // 2
    direct = min(DIRECT, half)
    upper, h = me // half, me % half
    far = partner(me, half)
    span = half * cap
    part = rows_in.shape[2]
    width = part * tiles
    count, channels = tokens.shape[1], w_proj.shape[1]
    n = len(pieces)
    turns = range(n)

    def rows(index, base=0):
        return pl.ds(pl.multiple_of(base + index * cap, cap), cap)

    peers = [(partner(me, k), partner(h, k)) for k in range(half)]
    block_of = [partner(h // direct, b) for b in range(half // direct)]

    def piece(j):
        begin, size = pieces[j]
        return slice(begin, begin + size)

    def columns(m, j):
        begin, size = pieces[j]
        return pl.ds(pl.multiple_of(m * part + begin, 128), size)

    def send(source, target, sent, arrived, device):
        pltpu.make_async_remote_copy(
            src_ref=source,
            dst_ref=target,
            send_sem=sent,
            recv_sem=arrived,
            device_id=device,
            device_id_type=MESH,
        ).start()

    def drain(block, sem):
        pltpu.make_async_copy(block, block, sem).wait()

    def some(j, number):
        return rows_in.at[0, pl.ds(0, number * cap), slice(None) if j is None else piece(j)]

    def many(j, number):
        return rows_in.at[:, pl.ds(0, number * cap), slice(None) if j is None else piece(j)]

    begin = pl.multiple_of(tile * part, part)
    sources = [(all_routes, routes), (all_gates, gates)]
    sources += [
        (all_tokens.at[:, m * part : (m + 1) * part], tokens.at[m]) for m in range(tiles)
    ]
    sources += [
        (all_cache, cache),
        (w_gate, gate_w),
        (w_up, up_w),
        (w_down, down_w),
        (all_time, w_time),
        (all_time_bias, bias_time),
        (all_space, w_space),
        (all_space_bias, bias_space),
        (all_proj.at[pl.ds(begin, part), :], w_proj),
        (all_gain.at[:, pl.ds(begin, part)], gain),
    ]
    loads = [
        pltpu.make_async_copy(source, held, load_sem.at[i])
        for i, (source, held) in enumerate(sources)
    ]
    for load in loads:
        load.start()
    token_loads, loads = loads[: 2 + tiles], loads[2 + tiles :]

    barrier = pltpu.get_barrier_semaphore()
    for k in range(1, half + 1):
        pl.semaphore_signal(barrier, inc=1, device_id=(partner(me, k), tile), device_id_type=MESH)
    for m in range(1, tiles):
        pl.semaphore_signal(
            barrier, inc=1, device_id=(me, (tile + m) % tiles), device_id_type=MESH
        )

    for load in token_loads[2:]:
        load.wait()
    pl.semaphore_wait(barrier, half + tiles - 1)

    def hand_over(j):
        here = piece(j)
        send(
            tokens.at[tile, :, here],
            relay_in.at[:, here],
            token_sem.at[n],
            token_sem.at[j],
            (far, tile),
        )

    token_loads[0].wait()
    token_loads[1].wait()
    expert = lax.broadcasted_iota(jnp.int32, (sessions, count), 0)
    named = [(routes[k : k + 1, :] == expert).astype(jnp.float32) for k in range(TOPK)]
    earlier = lax.broadcasted_iota(jnp.int32, (count, count), 0) < lax.broadcasted_iota(
        jnp.int32, (count, count), 1
    )
    before = jnp.dot(
        sum(named).astype(jnp.bfloat16),
        earlier.astype(jnp.float32).astype(jnp.bfloat16),
        preferred_element_type=jnp.float32,
    )
    targets = []
    for k in range(TOPK):
        place = jnp.sum(before * named[k], axis=0, keepdims=True).astype(jnp.int32)
        targets.append(routes[k : k + 1, :] * cap + place)
        before = before + named[k]
    weights = []
    for base, hot in ((upper * span, near_hot), ((1 - upper) * span, far_hot)):
        slot = base + lax.broadcasted_iota(jnp.int32, (span, count), 0)
        onehot = jnp.zeros((span, count), jnp.float32)
        weight = jnp.zeros((span, count), jnp.float32)
        for k in range(TOPK):
            hit = slot == targets[k]
            onehot = onehot + jnp.where(hit, 1.0, 0.0)
            weight = weight + jnp.where(hit, gates[k : k + 1, :], 0.0)
        hot[...] = onehot.astype(jnp.bfloat16)
        weights.append(weight)
    send(far_hot, hot_in, table_sem.at[0, 0], table_sem.at[1, 0], (far, tile))
    for j in turns:
        here = piece(j)
        for m in range(tiles):
            near_out[m, :, here] = jnp.dot(
                near_hot[...], tokens[m, :, here], preferred_element_type=jnp.float32
            ).astype(jnp.bfloat16)
        for k in range(half - 1, 0, -1):
            other, index = peers[k]
            if k < direct:
                source, target = near_out.at[:, rows(index), here], rows_in.at[:, rows(h), here]
                sems = direct_sem
            else:
                source = near_out.at[tile, rows(index), here]
                target = rows_in.at[tile, rows(h), here]
                sems = near_sem
            send(source, target, sems.at[n], sems.at[j], (other, tile))
        rows_in[:, rows(h), here] = near_out[:, rows(h), here]
    for j in turns:
        hand_over(j)
    for weight, mix in zip(weights, (near_mix, far_mix)):
        weight = weight.T
        high = weight.astype(jnp.bfloat16)
        mix[0] = high
        mix[1] = (weight - high.astype(jnp.float32)).astype(jnp.bfloat16)
    send(far_mix, mix_in, table_sem.at[0, 1], table_sem.at[1, 1], (far, tile))

    loads[0].wait()
    newest = head[0]
    slots = [cache[i] for i in range(3)]
    for t, shift in ((1, 0), (0, 2)):
        which = lax.rem(newest + shift, 3)
        past[t] = jnp.where(which == 0, slots[0], jnp.where(which == 1, slots[1], slots[2]))
    height = past.shape[1]
    for side, start, step in ((0, height - HALO, 1), (1, 0, tiles - 1)):
        send(
            past.at[:, start : start + HALO],
            halo.at[side],
            halo_sem.at[0, side],
            halo_sem.at[1, side],
            (me, (tile + step) % tiles),
        )

    def forward(block, sems, j):
        for m in range(1, tiles):
            send(block, block, sems.at[m, n], sems.at[m, j], (me, (tile + m) % tiles))

    def near_forward(j):
        drain(some(j, half - direct), near_sem.at[j])
        size = direct * cap
        for b in range(1, half // direct):
            begin = pl.multiple_of(block_of[b] * size, size)
            forward(rows_in.at[tile, pl.ds(begin, size), piece(j)], near_cross, j)

    def relay(j):
        here = piece(j)
        if j == 0:
            drain(hot_in, table_sem.at[1, 0])
        drain(relay_in.at[:, here], token_sem.at[j])
        relay_out[:, here] = jnp.dot(
            hot_in[...], relay_in[:, here], preferred_element_type=jnp.float32
        ).astype(jnp.bfloat16)
        for k in range(half - 1, 0, -1):
            other, index = peers[k]
            send(
                relay_out.at[rows(index), here],
                rows_in.at[tile, rows(h, span), here],
                far_sem.at[n],
                far_sem.at[j],
                (other, tile),
            )
        rows_in[tile, rows(h, span), here] = relay_out[rows(h), here]

    def far_forward(j):
        drain(some(j, half - 1), far_sem.at[j])
        forward(rows_in.at[tile, span : 2 * span, piece(j)], far_cross, j)

    def consume(group, j):
        base = group * span
        if group == 0:
            drain(many(j, direct - 1), direct_sem.at[j])
        for m in range(1, tiles):
            if group == 0:
                drain(some(j, half - direct), near_cross.at[m, j])
            else:
                drain(some(j, half), far_cross.at[m, j])
        if j == 0:
            gate[...] = jnp.zeros_like(gate)
            upward[...] = jnp.zeros_like(upward)

        for m in range(tiles):
            block = rows_in[m, base : base + span, piece(j)]
            gate[...] += across(block, gate_w[:, columns(m, j)])
            upward[...] += across(block, up_w[:, columns(m, j)])

    def activate(group):
        hidden[group] = (silu(gate[...]) * upward[...]).astype(jnp.bfloat16)

    def project(group, m, j):
        return jnp.dot(
            hidden[group], down_w[:, columns(m, j)], preferred_element_type=jnp.float32
        )

    def near_return(j):
        here = piece(j)

        for m in range(tiles):
            near_answer[m, :, here] = project(0, m, j).astype(jnp.bfloat16)

        for k in range(half - 1, 0, -1):
            other, index = peers[k]
            send(
                near_answer.at[:, rows(index), here],
                near_back.at[:, rows(h), here],
                back_sem.at[n],
                back_sem.at[j],
                (other, tile),
            )
        near_back[:, rows(h), here] = near_answer[:, rows(h), here]

    def blend(mix, block):
        return jnp.dot(mix[0], block, preferred_element_type=jnp.float32) + jnp.dot(
            mix[1], block, preferred_element_type=jnp.float32
        )

    def near_blend(j):
        here = piece(j)
        drain(many(j, half - 1), back_sem.at[j])
        for m in range(1, tiles):
            to = (tile + m) % tiles
            near_mixed[m - 1, :, here] = blend(near_mix, near_back[to, :, here]).astype(
                jnp.bfloat16
            )
            send(
                near_mixed.at[m - 1, :, here],
                mixed_in.at[m - 1, :, here],
                mixed_sem.at[m, n],
                mixed_sem.at[m, j],
                (me, to),
            )
        own_mixed[:, here] = blend(near_mix, near_back[tile, :, here])

    def far_answer(j):
        here = piece(j)
        for m in range(1, tiles):
            to = (tile + m) % tiles
            answer[m - 1, :, here] = project(1, to, j).astype(jnp.bfloat16)
            send(
                answer.at[m - 1, :, here],
                stage.at[m - 1, :, here],
                answer_sem.at[m, n],
                answer_sem.at[m, j],
                (me, to),
            )

    def far_return(j):
        here = piece(j)
        total = project(1, tile, j)
        for m in range(1, tiles):
            drain(stage.at[m - 1, :, here], answer_sem.at[m, j])
            total = total + stage[m - 1, :, here].astype(jnp.float32)
        reduced[:, here] = total.astype(jnp.bfloat16)
        for k in range(half - 1, 0, -1):
            other, index = peers[k]
            send(
                reduced.at[rows(index), here],
                back.at[rows(h), here],
                other_sem.at[n],
                other_sem.at[j],
                (other, tile),
            )
        back[rows(h), here] = reduced[rows(h), here]

    def far_blend(j):
        here = piece(j)
        if j == 0:
            drain(mix_in, table_sem.at[1, 1])
        drain(some(j, half - 1), other_sem.at[j])
        partial[:, here] = blend(mix_in, back[:, here]).astype(jnp.bfloat16)
        send(partial.at[:, here], summed.at[:, here], sum_sem.at[n], sum_sem.at[j], (far, tile))

    def features(j):
        here = piece(j)
        mixed = own_mixed[:, here]
        for m in range(1, tiles):
            drain(mixed_in.at[m - 1, :, here], mixed_sem.at[m, j])
            mixed = mixed + mixed_in[m - 1, :, here].astype(jnp.float32)
        drain(summed.at[:, here], sum_sem.at[j])
        mixed = mixed + summed[:, here].astype(jnp.float32)
        feat = (tokens[tile, :, here].astype(jnp.float32) + mixed).astype(jnp.bfloat16)
        feat = feat.astype(jnp.float32)
        scaled = (feat * gain[:, here]).astype(jnp.bfloat16)
        return (
            jnp.sum(feat * feat, axis=1, keepdims=True),
            jnp.dot(scaled, w_proj[here, :], preferred_element_type=jnp.float32),
        )

    tall = frames.shape[1]
    breadth = 2 * GRID_W
    edge = HALO * breadth
    pixels = out.shape[0]
    extended = pixels + 2 * breadth
    grid_rows = count // GRID_W
    own_rows = grid_rows // tiles

    def chosen(mask):
        return jnp.where(mask, 1.0, 0.0).astype(jnp.bfloat16)

    def moved(matrix, value):
        return jnp.dot(matrix, value, preferred_element_type=jnp.float32).astype(jnp.bfloat16)

    def shifts(size):
        to = lax.broadcasted_iota(jnp.int32, (size, size), 0)
        origin = lax.broadcasted_iota(jnp.int32, (size, size), 1)
        column = to % breadth
        return (
            chosen((origin == to - 1) & (column > 0)),
            chosen((origin == to + 1) & (column < breadth - 1)),
        )

    def widen(t, left, right):
        wide[t, :, :channels] = moved(left, frames[t])
        wide[t, :, channels : 2 * channels] = frames[t]
        wide[t, :, 2 * channels :] = moved(right, frames[t])

    def in_time(t):
        total = jnp.zeros((extended, channels), jnp.float32)
        for dy in range(3):
            total = total + jnp.dot(
                wide[t, dy * breadth : dy * breadth + extended, :],
                w_time[3 * t + dy],
                preferred_element_type=jnp.float32,
            )
        return total

    def earlier_frames():
        for side in range(2):
            drain(halo.at[side], halo_sem.at[1, side])
        left, right = shifts(tall)
        for t in range(2):
            top = halo[0, t].reshape(edge, channels)
            bottom = halo[1, t].reshape(edge, channels)
            frames[t, :edge, :] = jnp.where(tile > 0, top, jnp.zeros_like(top))
            frames[t, edge : edge + pixels, :] = past[t].reshape(pixels, channels)
            frames[t, edge + pixels :, :] = jnp.where(
                tile < tiles - 1, bottom, jnp.zeros_like(bottom)
            )
            widen(t, left, right)
        first[...] = in_time(0) + in_time(1) + bias_time[...]

    def last_frame():
        for r in range(own_rows + 2):
            row = tile * own_rows - 1 + r
            at = jnp.clip(row, 0, grid_rows - 1)
            value = coarse_in[pl.ds(pl.multiple_of(at * GRID_W, GRID_W), GRID_W), :]
            above[r * GRID_W : (r + 1) * GRID_W, :] = jnp.where(
                (row >= 0) & (row < grid_rows), value, jnp.zeros_like(value)
            )
        few = above.shape[0]
        pixel = lax.broadcasted_iota(jnp.int32, (tall, few), 0)
        token = lax.broadcasted_iota(jnp.int32, (tall, few), 1)
        spread = chosen(token == (pixel // (2 * breadth)) * GRID_W + (pixel % breadth) // 2)
        frames[2] = moved(spread, above[...].astype(jnp.bfloat16))
        left, right = shifts(tall)
        widen(2, left, right)
        total = first[...] + in_time(2)
        row = tile * (pixels // breadth) - 1 + lax.broadcasted_iota(
            jnp.int32, (extended, channels), 0
        ) // breadth
        inside = (row >= 0) & (row < tiles * (pixels // breadth))
        active = jnp.where(inside, silu(total), 0.0).astype(jnp.bfloat16)
        left, right = shifts(extended)
        wide_active[:, :channels] = moved(left, active)
        wide_active[:, channels : 2 * channels] = active
        wide_active[:, 2 * channels :] = moved(right, active)
        total = frames[2, edge : edge + pixels, :].astype(jnp.float32) + bias_space[...]
        for dy in range(3):
            total = total + jnp.dot(
                wide_active[dy * breadth : dy * breadth + pixels, :],
                w_space[dy],
                preferred_element_type=jnp.float32,
            )
        out[...] = total.astype(jnp.bfloat16)

    def steps(*stages):
        reach = n + max(lag for lag, _ in stages)
        for j in range(reach):
            for lag, stage_of in stages:
                if 0 <= j - lag < n:
                    stage_of(j - lag)

    for load in loads[1:3]:
        load.wait()
    late = max(n - 2, 0)
    for j in range(n + 1):
        if j < n:
            relay(j)
            near_forward(j)
        if j >= 1:
            consume(0, j - 1)
        if 0 <= j - 2 < late:
            far_forward(j - 2)
    activate(0)
    loads[3].wait()
    for j in turns:
        near_return(j)
        if late + j < n:
            far_forward(late + j)
    for load in loads[4:]:
        load.wait()
    earlier_frames()
    for j in turns:
        consume(1, j)
    activate(1)
    for j in turns:
        far_answer(j)
    found = []
    steps(
        (0, far_return),
        (0, near_blend),
        (1, far_blend),
        (2, lambda j: found.append(features(j))),
    )
    square = sum(pair[0] for pair in found)
    coarse = sum(pair[1] for pair in found)
    lane = lax.broadcasted_iota(jnp.int32, (count, 128), 1)
    high = square.astype(jnp.bfloat16).astype(jnp.float32)
    mine[:, :channels] = coarse.astype(jnp.bfloat16)
    mine[:, channels:] = jnp.where(
        lane == 0, high, jnp.where(lane == 1, square - high, 0.0)
    ).astype(jnp.bfloat16)
    for m in range(1, tiles):
        send(mine, theirs.at[m - 1], last_sem.at[0, m], last_sem.at[1, m], (me, (tile + m) % tiles))
    for m in range(1, tiles):
        drain(theirs.at[m - 1], last_sem.at[1, m])
        coarse = coarse + theirs[m - 1, :, :channels].astype(jnp.float32)
        square = square + jnp.sum(
            theirs[m - 1, :, channels:].astype(jnp.float32), axis=1, keepdims=True
        )
    coarse_in[...] = coarse * lax.rsqrt(square * (1.0 / width) + epsilon)
    last_frame()

    drain(far_hot, table_sem.at[0, 0])
    drain(far_mix, table_sem.at[0, 1])
    for side in range(2):
        drain(halo.at[side], halo_sem.at[0, side])
    drain(relay_in, token_sem.at[n])
    drain(some(None, half - direct), near_sem.at[n])
    drain(many(None, direct - 1), direct_sem.at[n])
    drain(some(None, half - 1), far_sem.at[n])
    drain(many(None, half - 1), back_sem.at[n])
    drain(some(None, half - 1), other_sem.at[n])
    drain(summed, sum_sem.at[n])
    for m in range(1, tiles):
        drain(some(None, half - direct), near_cross.at[m, n])
        drain(some(None, half), far_cross.at[m, n])
        drain(mixed_in.at[m - 1], mixed_sem.at[m, n])
        drain(stage.at[m - 1], answer_sem.at[m, n])
        drain(theirs.at[m - 1], last_sem.at[0, m])


def layer(
    routes,
    gates,
    head,
    gain,
    tokens,
    w_gate,
    w_up,
    w_down,
    w_proj,
    cache,
    w_time,
    bias_time,
    w_space,
    bias_space,
    sizes,
):
    sessions, tiles, cap = sizes
    count, width = tokens.shape
    hid, part, half = w_gate.shape[0], width // tiles, sessions // 2
    span, channels = half * cap, w_proj.shape[1]
    pixels = cache.shape[1] * cache.shape[2]
    breadth = 2 * GRID_W
    tall = pixels + 2 * HALO * breadth
    few = count // tiles + 2 * GRID_W
    pieces = pieces_of(part)
    hbm = pl.BlockSpec(memory_space=pltpu.HBM)
    low, full = jnp.bfloat16, jnp.float32
    n = len(pieces)
    held = [
        (routes.shape, routes.dtype),
        (gates.shape, full),
        ((1, part), full),
        ((tiles, count, part), low),
        (w_gate.shape, low),
        (w_up.shape, low),
        (w_down.shape, low),
        ((part, channels), low),
        (cache.shape, low),
        (w_time.shape, low),
        (bias_time.shape, full),
        (w_space.shape, low),
        (bias_space.shape, full),
        ((2,) + cache.shape[1:], low),
        ((2, 2, HALO) + cache.shape[2:], low),
        ((span, count), low),
        ((span, count), low),
        ((2, count, span), low),
        ((2, count, span), low),
        ((span, count), low),
        ((2, count, span), low),
        ((count, part), low),
        ((tiles, span, part), low),
        ((span, part), low),
        ((tiles, 2 * span, part), low),
        ((span, hid), full),
        ((span, hid), full),
        ((2, span, hid), low),
        ((tiles, span, part), low),
        ((tiles, span, part), low),
        ((tiles - 1, count, part), low),
        ((count, part), full),
        ((tiles - 1, count, part), low),
        ((tiles - 1, span, part), low),
        ((tiles - 1, span, part), low),
        ((span, part), low),
        ((span, part), low),
        ((count, part), low),
        ((count, part), low),
        ((count, channels + 128), low),
        ((tiles - 1, count, channels + 128), low),
        ((count, channels), full),
        ((few, channels), full),
        ((3, tall, channels), low),
        ((3, tall, 3 * channels), low),
        ((pixels + 2 * breadth, channels), full),
        ((pixels + 2 * breadth, 3 * channels), low),
    ]
    sems = [
        (12 + tiles,),
        (2, 2),
        (2, 2),
        (n + 1,),
        (n + 1,),
        (n + 1,),
        (n + 1,),
        (tiles, n + 1),
        (tiles, n + 1),
        (n + 1,),
        (tiles, n + 1),
        (tiles, n + 1),
        (n + 1,),
        (n + 1,),
        (2, tiles),
    ]
    return pl.pallas_call(
        functools.partial(layer_kernel, sessions, tiles, cap, pieces),
        out_shape=jax.ShapeDtypeStruct((pixels, channels), low),
        in_specs=[hbm, hbm, pl.BlockSpec(memory_space=pltpu.SMEM)] + [hbm] * 11,
        out_specs=VMEM,
        scratch_shapes=[pltpu.VMEM(*each) for each in held]
        + [pltpu.SemaphoreType.DMA(each) for each in sems],
        compiler_params=pltpu.CompilerParams(
            collective_id=0, has_side_effects=True, vmem_limit_bytes=60 * 2**20
        ),
        name="layer",
    )(
        routes,
        gates,
        head,
        gain,
        tokens,
        w_gate,
        w_up,
        w_down,
        w_proj,
        cache,
        w_time,
        bias_time,
        w_space,
        bias_space,
    )


def body(
    tokens,
    routes,
    gates,
    w_gate,
    w_up,
    w_down,
    feat_gain,
    w_proj,
    conv_time,
    bias_time,
    conv_space,
    bias_space,
    frame_cache,
    cache_head,
):
    sessions, tiles = lax.axis_size("sess"), lax.axis_size("exp")
    channels = w_proj.shape[-1]
    local = tokens[0]
    tok_count = local.shape[0]
    cap = 2 * tok_count * TOPK // sessions
    height, breadth = frame_cache.shape[2:4]
    result = layer(
        routes[0].T,
        gates[0].T,
        cache_head,
        feat_gain[None, :],
        local,
        w_gate[0].T,
        w_up[0].T,
        w_down[0],
        w_proj,
        frame_cache[:, 0],
        conv_time.reshape(9, 3 * channels, channels),
        bias_time[None, :],
        conv_space.reshape(3, 3 * channels, channels),
        bias_space[None, :],
        (sessions, tiles, cap),
    )
    return result.reshape(1, height, breadth, channels)


def solution(mesh):
    return jax.shard_map(
        body,
        mesh=mesh,
        in_specs=(
            P("sess", None, None),
            P("sess", None, None),
            P("sess", None, None),
            P("sess", None, "exp"),
            P("sess", None, "exp"),
            P("sess", "exp", None),
            P(),
            P(),
            P(),
            P(),
            P(),
            P(),
            P(None, "sess", "exp", None, None),
            P("sess"),
        ),
        out_specs=P("sess", "exp", None, None),
        check_vma=False,
    )
```

```python
import functools

import jax
import jax.numpy as jnp
from jax import lax
from jax.experimental import pallas as pl
from jax.experimental.pallas import tpu as pltpu
from jax.sharding import PartitionSpec as P

TOPK = 2
GRID_W = 8
HALO = 2
DIRECT = 4
MESH = pl.DeviceIdType.MESH
VMEM = pl.BlockSpec(memory_space=pltpu.VMEM)

epsilon = 1e-06


def partner(me, bits):
    other, weight = me, 1
    while bits:
        if bits & 1:
            other = other + weight * (1 - 2 * ((me // weight) % 2))
        bits //= 2
        weight *= 2
    return other


def silu(value):
    return value / (1.0 + jnp.exp(-value))


def across(left, right):
    return lax.dot_general(
        left, right, (((1,), (1,)), ((), ())), preferred_element_type=jnp.float32
    )


def pieces_of(part):
    size = max(128, part // 4)
    return [(begin, size) for begin in range(0, part, size)]


def fine_of(part, n):
    return 2 if part // n % 256 == 0 else 1


def layer_kernel(
    sessions,
    tiles,
    cap,
    pieces,
    all_routes,
    all_gates,
    head,
    all_gain,
    all_tokens,
    w_gate,
    w_up,
    w_down,
    all_proj,
    all_cache,
    all_time,
    all_time_bias,
    all_space,
    all_space_bias,
    out,
    routes,
    gates,
    gain,
    tokens,
    gate_w,
    up_w,
    down_w,
    w_proj,
    cache,
    w_time,
    bias_time,
    w_space,
    bias_space,
    past,
    halo,
    near_hot,
    far_hot,
    near_mix,
    far_mix,
    hot_in,
    mix_in,
    relay_in,
    near_out,
    relay_out,
    rows_in,
    gate,
    upward,
    hidden,
    near_answer,
    near_back,
    near_mixed,
    own_mixed,
    mixed_in,
    answer,
    stage,
    reduced,
    back,
    partial,
    summed,
    mine,
    theirs,
    coarse_in,
    above,
    frames,
    wide,
    first,
    wide_active,
    load_sem,
    halo_sem,
    table_sem,
    token_sem,
    near_sem,
    direct_sem,
    far_sem,
    near_cross,
    far_cross,
    back_sem,
    mixed_sem,
    answer_sem,
    other_sem,
    sum_sem,
    last_sem,
):
    me, tile = lax.axis_index("sess"), lax.axis_index("exp")
    half = sessions // 2
    direct = min(DIRECT, half)
    upper, h = me // half, me % half
    far = partner(me, half)
    span = half * cap
    part = rows_in.shape[2]
    width = part * tiles
    count, channels = tokens.shape[1], w_proj.shape[1]
    n = len(pieces)
    turns = range(n)
    split = fine_of(part, n)
    parts = range(n * split)

    def rows(index, base=0):
        return pl.ds(pl.multiple_of(base + index * cap, cap), cap)

    peers = [(partner(me, k), partner(h, k)) for k in range(half)]
    block_of = [partner(h // direct, b) for b in range(half // direct)]

    def piece(j):
        begin, size = pieces[j]
        return slice(begin, begin + size)

    def columns(m, j):
        begin, size = pieces[j]
        return pl.ds(pl.multiple_of(m * part + begin, 128), size)

    def fine(j):
        size = part // len(parts)
        return slice(j * size, (j + 1) * size)

    def send(source, target, sent, arrived, device):
        pltpu.make_async_remote_copy(
            src_ref=source,
            dst_ref=target,
            send_sem=sent,
            recv_sem=arrived,
            device_id=device,
            device_id_type=MESH,
        ).start()

    def drain(block, sem):
        pltpu.make_async_copy(block, block, sem).wait()

    def some(j, number):
        return rows_in.at[0, pl.ds(0, number * cap), slice(None) if j is None else piece(j)]

    def many(j, number):
        return rows_in.at[:, pl.ds(0, number * cap), slice(None) if j is None else piece(j)]

    begin = pl.multiple_of(tile * part, part)
    sources = [(all_routes, routes), (all_gates, gates)]
    sources += [
        (all_tokens.at[:, m * part : (m + 1) * part], tokens.at[m]) for m in range(tiles)
    ]
    sources += [
        (all_cache, cache),
        (w_gate, gate_w),
        (w_up, up_w),
        (w_down, down_w),
        (all_time, w_time),
        (all_time_bias, bias_time),
        (all_space, w_space),
        (all_space_bias, bias_space),
        (all_proj.at[pl.ds(begin, part), :], w_proj),
        (all_gain.at[:, pl.ds(begin, part)], gain),
    ]
    loads = [
        pltpu.make_async_copy(source, held, load_sem.at[i])
        for i, (source, held) in enumerate(sources)
    ]
    for load in loads:
        load.start()
    token_loads, loads = loads[: 2 + tiles], loads[2 + tiles :]

    barrier = pltpu.get_barrier_semaphore()
    for k in range(1, half + 1):
        pl.semaphore_signal(barrier, inc=1, device_id=(partner(me, k), tile), device_id_type=MESH)
    for m in range(1, tiles):
        pl.semaphore_signal(
            barrier, inc=1, device_id=(me, (tile + m) % tiles), device_id_type=MESH
        )

    token_loads[0].wait()
    token_loads[1].wait()
    expert = lax.broadcasted_iota(jnp.int32, (sessions, count), 0)
    named = [(routes[k : k + 1, :] == expert).astype(jnp.float32) for k in range(TOPK)]
    earlier = lax.broadcasted_iota(jnp.int32, (count, count), 0) < lax.broadcasted_iota(
        jnp.int32, (count, count), 1
    )
    before = jnp.dot(
        sum(named).astype(jnp.bfloat16),
        earlier.astype(jnp.float32).astype(jnp.bfloat16),
        preferred_element_type=jnp.float32,
    )
    targets = []
    for k in range(TOPK):
        place = jnp.sum(before * named[k], axis=0, keepdims=True).astype(jnp.int32)
        targets.append(routes[k : k + 1, :] * cap + place)
        before = before + named[k]
    weights = []
    for base, hot in ((upper * span, near_hot), ((1 - upper) * span, far_hot)):
        slot = base + lax.broadcasted_iota(jnp.int32, (span, count), 0)
        onehot = jnp.zeros((span, count), jnp.float32)
        weight = jnp.zeros((span, count), jnp.float32)
        for k in range(TOPK):
            hit = slot == targets[k]
            onehot = onehot + jnp.where(hit, 1.0, 0.0)
            weight = weight + jnp.where(hit, gates[k : k + 1, :], 0.0)
        hot[...] = onehot.astype(jnp.bfloat16)
        weights.append(weight)
    for weight, mix in zip(weights, (near_mix, far_mix)):
        weight = weight.T
        high = weight.astype(jnp.bfloat16)
        mix[0] = high
        mix[1] = (weight - high.astype(jnp.float32)).astype(jnp.bfloat16)
    for load in token_loads[2:]:
        load.wait()
    for j in turns:
        for m in range(tiles):
            near_out[m, :, piece(j)] = jnp.dot(
                near_hot[...], tokens[m, :, piece(j)], preferred_element_type=jnp.float32
            ).astype(jnp.bfloat16)
    rows_in[:, rows(h), :] = near_out[:, rows(h), :]
    loads[0].wait()
    newest = head[0]
    slots = [cache[i] for i in range(3)]
    for t, shift in ((1, 0), (0, 2)):
        which = lax.rem(newest + shift, 3)
        past[t] = jnp.where(which == 0, slots[0], jnp.where(which == 1, slots[1], slots[2]))
    pl.semaphore_wait(barrier, half + tiles - 1)

    def hand_over(j):
        here = piece(j)
        send(
            tokens.at[tile, :, here],
            relay_in.at[:, here],
            token_sem.at[n],
            token_sem.at[j],
            (far, tile),
        )

    send(far_hot, hot_in, table_sem.at[0, 0], table_sem.at[1, 0], (far, tile))
    for j in turns:
        here = piece(j)
        for k in range(half - 1, 0, -1):
            other, index = peers[k]
            if k < direct:
                source, target = near_out.at[:, rows(index), here], rows_in.at[:, rows(h), here]
                sems = direct_sem
            else:
                source = near_out.at[tile, rows(index), here]
                target = rows_in.at[tile, rows(h), here]
                sems = near_sem
            send(source, target, sems.at[n], sems.at[j], (other, tile))
    for j in turns:
        hand_over(j)
    send(far_mix, mix_in, table_sem.at[0, 1], table_sem.at[1, 1], (far, tile))

    height = past.shape[1]
    for side, start, step in ((0, height - HALO, 1), (1, 0, tiles - 1)):
        send(
            past.at[:, start : start + HALO],
            halo.at[side],
            halo_sem.at[0, side],
            halo_sem.at[1, side],
            (me, (tile + step) % tiles),
        )

    def forward(block, sems, j):
        for m in range(1, tiles):
            send(block, block, sems.at[m, n], sems.at[m, j], (me, (tile + m) % tiles))

    def near_forward(j):
        drain(some(j, half - direct), near_sem.at[j])
        size = direct * cap
        for b in range(1, half // direct):
            begin = pl.multiple_of(block_of[b] * size, size)
            forward(rows_in.at[tile, pl.ds(begin, size), piece(j)], near_cross, j)

    def relay(j):
        here = piece(j)
        if j == 0:
            drain(hot_in, table_sem.at[1, 0])
        drain(relay_in.at[:, here], token_sem.at[j])
        relay_out[:, here] = jnp.dot(
            hot_in[...], relay_in[:, here], preferred_element_type=jnp.float32
        ).astype(jnp.bfloat16)
        for k in range(half - 1, 0, -1):
            other, index = peers[k]
            send(
                relay_out.at[rows(index), here],
                rows_in.at[tile, rows(h, span), here],
                far_sem.at[n],
                far_sem.at[j],
                (other, tile),
            )
        rows_in[tile, rows(h, span), here] = relay_out[rows(h), here]

    def far_forward(j):
        drain(some(j, half - 1), far_sem.at[j])
        forward(rows_in.at[tile, span : 2 * span, piece(j)], far_cross, j)

    def consume(group, j):
        base = group * span
        if group == 0:
            drain(many(j, direct - 1), direct_sem.at[j])
        for m in range(1, tiles):
            if group == 0:
                drain(some(j, half - direct), near_cross.at[m, j])
            else:
                drain(some(j, half), far_cross.at[m, j])
        if j == 0:
            gate[...] = jnp.zeros_like(gate)
            upward[...] = jnp.zeros_like(upward)

        for m in range(tiles):
            block = rows_in[m, base : base + span, piece(j)]
            gate[...] += across(block, gate_w[:, columns(m, j)])
            upward[...] += across(block, up_w[:, columns(m, j)])

    def activate(group):
        hidden[group] = (silu(gate[...]) * upward[...]).astype(jnp.bfloat16)

    def project(group, m, here):
        span_in = pl.ds(pl.multiple_of(m * part + here.start, 128), here.stop - here.start)
        return jnp.dot(hidden[group], down_w[:, span_in], preferred_element_type=jnp.float32)

    def near_return(j):
        here = piece(j)

        for m in range(tiles):
            near_answer[m, :, here] = project(0, m, here).astype(jnp.bfloat16)

        for k in range(half - 1, 0, -1):
            other, index = peers[k]
            send(
                near_answer.at[:, rows(index), here],
                near_back.at[:, rows(h), here],
                back_sem.at[n],
                back_sem.at[j],
                (other, tile),
            )
        near_back[:, rows(h), here] = near_answer[:, rows(h), here]

    def blend(mix, block):
        return jnp.dot(mix[0], block, preferred_element_type=jnp.float32) + jnp.dot(
            mix[1], block, preferred_element_type=jnp.float32
        )

    def near_blend(j):
        here = piece(j)
        drain(many(j, half - 1), back_sem.at[j])
        for m in range(1, tiles):
            to = (tile + m) % tiles
            near_mixed[m - 1, :, here] = blend(near_mix, near_back[to, :, here]).astype(
                jnp.bfloat16
            )
            send(
                near_mixed.at[m - 1, :, here],
                mixed_in.at[m - 1, :, here],
                mixed_sem.at[m, n],
                mixed_sem.at[m, j],
                (me, to),
            )
        own_mixed[:, here] = blend(near_mix, near_back[tile, :, here])

    def far_answer(j):
        here = fine(j)
        for m in range(1, tiles):
            to = (tile + m) % tiles
            answer[m - 1, :, here] = project(1, to, here).astype(jnp.bfloat16)
            send(
                answer.at[m - 1, :, here],
                stage.at[m - 1, :, here],
                answer_sem.at[m, n * split],
                answer_sem.at[m, j],
                (me, to),
            )

    def far_return(j):
        here = fine(j)
        total = project(1, tile, here)
        for m in range(1, tiles):
            drain(stage.at[m - 1, :, here], answer_sem.at[m, j])
            total = total + stage[m - 1, :, here].astype(jnp.float32)
        reduced[:, here] = total.astype(jnp.bfloat16)
        for k in range(half - 1, 0, -1):
            other, index = peers[k]
            send(
                reduced.at[rows(index), here],
                back.at[rows(h), here],
                other_sem.at[n * split],
                other_sem.at[j],
                (other, tile),
            )
        back[rows(h), here] = reduced[rows(h), here]

    def far_blend(j):
        here = fine(j)
        if j == 0:
            drain(mix_in, table_sem.at[1, 1])
        drain(rows_in.at[0, pl.ds(0, (half - 1) * cap), here], other_sem.at[j])
        partial[:, here] = blend(mix_in, back[:, here]).astype(jnp.bfloat16)
        send(partial.at[:, here], summed.at[:, here], sum_sem.at[n * split], sum_sem.at[j], (far, tile))

    def features(j):
        here = fine(j)
        mixed = own_mixed[:, here]
        for m in range(1, tiles):
            if j % split == 0:
                whole = piece(j // split)
                drain(mixed_in.at[m - 1, :, whole], mixed_sem.at[m, j // split])
            mixed = mixed + mixed_in[m - 1, :, here].astype(jnp.float32)
        drain(summed.at[:, here], sum_sem.at[j])
        mixed = mixed + summed[:, here].astype(jnp.float32)
        feat = (tokens[tile, :, here].astype(jnp.float32) + mixed).astype(jnp.bfloat16)
        feat = feat.astype(jnp.float32)
        scaled = (feat * gain[:, here]).astype(jnp.bfloat16)
        return (
            jnp.sum(feat * feat, axis=1, keepdims=True),
            jnp.dot(scaled, w_proj[here, :], preferred_element_type=jnp.float32),
        )

    tall = frames.shape[1]
    breadth = 2 * GRID_W
    edge = HALO * breadth
    pixels = out.shape[0]
    extended = pixels + 2 * breadth
    grid_rows = count // GRID_W
    own_rows = grid_rows // tiles

    def chosen(mask):
        return jnp.where(mask, 1.0, 0.0).astype(jnp.bfloat16)

    def moved(matrix, value):
        return jnp.dot(matrix, value, preferred_element_type=jnp.float32).astype(jnp.bfloat16)

    def shifts(size):
        to = lax.broadcasted_iota(jnp.int32, (size, size), 0)
        origin = lax.broadcasted_iota(jnp.int32, (size, size), 1)
        column = to % breadth
        return (
            chosen((origin == to - 1) & (column > 0)),
            chosen((origin == to + 1) & (column < breadth - 1)),
        )

    def widen(t, left, right):
        wide[t, :, :channels] = moved(left, frames[t])
        wide[t, :, channels : 2 * channels] = frames[t]
        wide[t, :, 2 * channels :] = moved(right, frames[t])

    def in_time(t):
        total = jnp.zeros((extended, channels), jnp.float32)
        for dy in range(3):
            total = total + jnp.dot(
                wide[t, dy * breadth : dy * breadth + extended, :],
                w_time[3 * t + dy],
                preferred_element_type=jnp.float32,
            )
        return total

    def earlier_frames():
        for side in range(2):
            drain(halo.at[side], halo_sem.at[1, side])
        left, right = shifts(tall)
        for t in range(2):
            top = halo[0, t].reshape(edge, channels)
            bottom = halo[1, t].reshape(edge, channels)
            frames[t, :edge, :] = jnp.where(tile > 0, top, jnp.zeros_like(top))
            frames[t, edge : edge + pixels, :] = past[t].reshape(pixels, channels)
            frames[t, edge + pixels :, :] = jnp.where(
                tile < tiles - 1, bottom, jnp.zeros_like(bottom)
            )
            widen(t, left, right)
        first[...] = in_time(0) + in_time(1) + bias_time[...]

    def last_frame():
        for r in range(own_rows + 2):
            row = tile * own_rows - 1 + r
            at = jnp.clip(row, 0, grid_rows - 1)
            value = coarse_in[pl.ds(pl.multiple_of(at * GRID_W, GRID_W), GRID_W), :]
            above[r * GRID_W : (r + 1) * GRID_W, :] = jnp.where(
                (row >= 0) & (row < grid_rows), value, jnp.zeros_like(value)
            )
        few = above.shape[0]
        pixel = lax.broadcasted_iota(jnp.int32, (tall, few), 0)
        token = lax.broadcasted_iota(jnp.int32, (tall, few), 1)
        spread = chosen(token == (pixel // (2 * breadth)) * GRID_W + (pixel % breadth) // 2)
        frames[2] = moved(spread, above[...].astype(jnp.bfloat16))
        left, right = shifts(tall)
        widen(2, left, right)
        total = first[...] + in_time(2)
        row = tile * (pixels // breadth) - 1 + lax.broadcasted_iota(
            jnp.int32, (extended, channels), 0
        ) // breadth
        inside = (row >= 0) & (row < tiles * (pixels // breadth))
        active = jnp.where(inside, silu(total), 0.0).astype(jnp.bfloat16)
        left, right = shifts(extended)
        wide_active[:, :channels] = moved(left, active)
        wide_active[:, channels : 2 * channels] = active
        wide_active[:, 2 * channels :] = moved(right, active)
        total = frames[2, edge : edge + pixels, :].astype(jnp.float32) + bias_space[...]
        for dy in range(3):
            total = total + jnp.dot(
                wide_active[dy * breadth : dy * breadth + pixels, :],
                w_space[dy],
                preferred_element_type=jnp.float32,
            )
        out[...] = total.astype(jnp.bfloat16)

    for load in loads[1:3]:
        load.wait()
    for j in range(n + 3):
        if j < n:
            relay(j)
            near_forward(j)
        if 0 <= j - 2 < n:
            consume(0, j - 2)
        if 0 <= j - 3:
            far_forward(j - 3)
    activate(0)
    loads[3].wait()
    for j in turns:
        near_return(j)
    for load in loads[4:]:
        load.wait()
    earlier_frames()
    for j in turns:
        consume(1, j)
    activate(1)
    for j in parts:
        far_answer(j)
    found = []
    for j in range(len(parts) + 6):
        if j < len(parts):
            far_return(j)
            if j % split == 0:
                near_blend(j // split)
        if 0 <= j - 2 < len(parts):
            far_blend(j - 2)
        if 0 <= j - 6:
            found.append(features(j - 6))
    square = sum(pair[0] for pair in found)
    coarse = sum(pair[1] for pair in found)
    lane = lax.broadcasted_iota(jnp.int32, (count, 128), 1)
    high = square.astype(jnp.bfloat16).astype(jnp.float32)
    mine[:, :channels] = coarse.astype(jnp.bfloat16)
    mine[:, channels:] = jnp.where(
        lane == 0, high, jnp.where(lane == 1, square - high, 0.0)
    ).astype(jnp.bfloat16)
    for m in range(1, tiles):
        send(mine, theirs.at[m - 1], last_sem.at[0, m], last_sem.at[1, m], (me, (tile + m) % tiles))
    for m in range(1, tiles):
        drain(theirs.at[m - 1], last_sem.at[1, m])
        coarse = coarse + theirs[m - 1, :, :channels].astype(jnp.float32)
        square = square + jnp.sum(
            theirs[m - 1, :, channels:].astype(jnp.float32), axis=1, keepdims=True
        )
    coarse_in[...] = coarse * lax.rsqrt(square * (1.0 / width) + epsilon)
    last_frame()

    drain(far_hot, table_sem.at[0, 0])
    drain(far_mix, table_sem.at[0, 1])
    for side in range(2):
        drain(halo.at[side], halo_sem.at[0, side])
    drain(relay_in, token_sem.at[n])
    drain(some(None, half - direct), near_sem.at[n])
    drain(many(None, direct - 1), direct_sem.at[n])
    drain(some(None, half - 1), far_sem.at[n])
    drain(many(None, half - 1), back_sem.at[n])
    drain(some(None, half - 1), other_sem.at[n * split])
    drain(summed, sum_sem.at[n * split])
    for m in range(1, tiles):
        drain(some(None, half - direct), near_cross.at[m, n])
        drain(some(None, half), far_cross.at[m, n])
        drain(mixed_in.at[m - 1], mixed_sem.at[m, n])
        drain(stage.at[m - 1], answer_sem.at[m, n * split])
        drain(theirs.at[m - 1], last_sem.at[0, m])


def layer(
    routes,
    gates,
    head,
    gain,
    tokens,
    w_gate,
    w_up,
    w_down,
    w_proj,
    cache,
    w_time,
    bias_time,
    w_space,
    bias_space,
    sizes,
):
    sessions, tiles, cap = sizes
    count, width = tokens.shape
    hid, part, half = w_gate.shape[0], width // tiles, sessions // 2
    span, channels = half * cap, w_proj.shape[1]
    pixels = cache.shape[1] * cache.shape[2]
    breadth = 2 * GRID_W
    tall = pixels + 2 * HALO * breadth
    few = count // tiles + 2 * GRID_W
    pieces = pieces_of(part)
    hbm = pl.BlockSpec(memory_space=pltpu.HBM)
    low, full = jnp.bfloat16, jnp.float32
    n = len(pieces)
    split = fine_of(part, n)
    held = [
        (routes.shape, routes.dtype),
        (gates.shape, full),
        ((1, part), full),
        ((tiles, count, part), low),
        (w_gate.shape, low),
        (w_up.shape, low),
        (w_down.shape, low),
        ((part, channels), low),
        (cache.shape, low),
        (w_time.shape, low),
        (bias_time.shape, full),
        (w_space.shape, low),
        (bias_space.shape, full),
        ((2,) + cache.shape[1:], low),
        ((2, 2, HALO) + cache.shape[2:], low),
        ((span, count), low),
        ((span, count), low),
        ((2, count, span), low),
        ((2, count, span), low),
        ((span, count), low),
        ((2, count, span), low),
        ((count, part), low),
        ((tiles, span, part), low),
        ((span, part), low),
        ((tiles, 2 * span, part), low),
        ((span, hid), full),
        ((span, hid), full),
        ((2, span, hid), low),
        ((tiles, span, part), low),
        ((tiles, span, part), low),
        ((tiles - 1, count, part), low),
        ((count, part), full),
        ((tiles - 1, count, part), low),
        ((tiles - 1, span, part), low),
        ((tiles - 1, span, part), low),
        ((span, part), low),
        ((span, part), low),
        ((count, part), low),
        ((count, part), low),
        ((count, channels + 128), low),
        ((tiles - 1, count, channels + 128), low),
        ((count, channels), full),
        ((few, channels), full),
        ((3, tall, channels), low),
        ((3, tall, 3 * channels), low),
        ((pixels + 2 * breadth, channels), full),
        ((pixels + 2 * breadth, 3 * channels), low),
    ]
    sems = [
        (12 + tiles,),
        (2, 2),
        (2, 2),
        (n + 1,),
        (n + 1,),
        (n + 1,),
        (n + 1,),
        (tiles, n + 1),
        (tiles, n + 1),
        (n + 1,),
        (tiles, n + 1),
        (tiles, n * split + 1),
        (n * split + 1,),
        (n * split + 1,),
        (2, tiles),
    ]
    return pl.pallas_call(
        functools.partial(layer_kernel, sessions, tiles, cap, pieces),
        out_shape=jax.ShapeDtypeStruct((pixels, channels), low),
        in_specs=[hbm, hbm, pl.BlockSpec(memory_space=pltpu.SMEM)] + [hbm] * 11,
        out_specs=VMEM,
        scratch_shapes=[pltpu.VMEM(*each) for each in held]
        + [pltpu.SemaphoreType.DMA(each) for each in sems],
        compiler_params=pltpu.CompilerParams(
            collective_id=0, has_side_effects=True, vmem_limit_bytes=60 * 2**20
        ),
        name="layer",
    )(
        routes,
        gates,
        head,
        gain,
        tokens,
        w_gate,
        w_up,
        w_down,
        w_proj,
        cache,
        w_time,
        bias_time,
        w_space,
        bias_space,
    )


def body(
    tokens,
    routes,
    gates,
    w_gate,
    w_up,
    w_down,
    feat_gain,
    w_proj,
    conv_time,
    bias_time,
    conv_space,
    bias_space,
    frame_cache,
    cache_head,
):
    sessions, tiles = lax.axis_size("sess"), lax.axis_size("exp")
    channels = w_proj.shape[-1]
    local = tokens[0]
    tok_count = local.shape[0]
    cap = 2 * tok_count * TOPK // sessions
    height, breadth = frame_cache.shape[2:4]
    result = layer(
        routes[0].T,
        gates[0].T,
        cache_head,
        feat_gain[None, :],
        local,
        w_gate[0].T,
        w_up[0].T,
        w_down[0],
        w_proj,
        frame_cache[:, 0],
        conv_time.reshape(9, 3 * channels, channels),
        bias_time[None, :],
        conv_space.reshape(3, 3 * channels, channels),
        bias_space[None, :],
        (sessions, tiles, cap),
    )
    return result.reshape(1, height, breadth, channels)


def solution(mesh):
    return jax.shard_map(
        body,
        mesh=mesh,
        in_specs=(
            P("sess", None, None),
            P("sess", None, None),
            P("sess", None, None),
            P("sess", None, "exp"),
            P("sess", None, "exp"),
            P("sess", "exp", None),
            P(),
            P(),
            P(),
            P(),
            P(),
            P(),
            P(None, "sess", "exp", None, None),
            P("sess"),
        ),
        out_specs=P("sess", "exp", None, None),
        check_vma=False,
    )
```

```python
import functools

import jax
import jax.numpy as jnp
from jax import lax
from jax.experimental import pallas as pl
from jax.experimental.pallas import tpu as pltpu
from jax.sharding import PartitionSpec as P

TOPK = 2
GRID_W = 8
HALO = 2
DIRECT = 4
MESH = pl.DeviceIdType.MESH
VMEM = pl.BlockSpec(memory_space=pltpu.VMEM)

epsilon = 1e-06


def partner(me, bits):
    other, weight = me, 1
    while bits:
        if bits & 1:
            other = other + weight * (1 - 2 * ((me // weight) % 2))
        bits //= 2
        weight *= 2
    return other


def silu(value):
    return value / (1.0 + jnp.exp(-value))


def across(left, right):
    return lax.dot_general(
        left, right, (((1,), (1,)), ((), ())), preferred_element_type=jnp.float32
    )


def pieces_of(part):
    size = max(128, part // 4)
    return [(begin, size) for begin in range(0, part, size)]


def fine_of(part, n):
    return 2 if part // n % 256 == 0 else 1


def layer_kernel(
    sessions,
    tiles,
    cap,
    pieces,
    all_routes,
    all_gates,
    head,
    all_gain,
    all_tokens,
    w_gate,
    w_up,
    w_down,
    all_proj,
    all_cache,
    all_time,
    all_time_bias,
    all_space,
    all_space_bias,
    out,
    routes,
    gates,
    gain,
    tokens,
    gate_w,
    up_w,
    down_w,
    w_proj,
    cache,
    w_time,
    bias_time,
    w_space,
    bias_space,
    past,
    halo,
    near_hot,
    far_hot,
    near_mix,
    far_mix,
    hot_in,
    mix_in,
    relay_in,
    near_out,
    relay_out,
    rows_in,
    gate,
    upward,
    hidden,
    near_answer,
    near_back,
    near_mixed,
    own_mixed,
    mixed_in,
    answer,
    stage,
    reduced,
    back,
    partial,
    summed,
    mine,
    theirs,
    coarse_in,
    above,
    frames,
    wide,
    first,
    wide_active,
    load_sem,
    halo_sem,
    table_sem,
    token_sem,
    near_sem,
    direct_sem,
    far_sem,
    near_cross,
    far_cross,
    back_sem,
    mixed_sem,
    answer_sem,
    other_sem,
    sum_sem,
    last_sem,
):
    me, tile = lax.axis_index("sess"), lax.axis_index("exp")
    half = sessions // 2
    direct = min(DIRECT, half)
    upper, h = me // half, me % half
    far = partner(me, half)
    span = half * cap
    part = rows_in.shape[2]
    width = part * tiles
    count, channels = tokens.shape[1], w_proj.shape[1]
    n = len(pieces)
    turns = range(n)
    split = fine_of(part, n)
    parts = range(n * split)

    def rows(index, base=0):
        return pl.ds(pl.multiple_of(base + index * cap, cap), cap)

    peers = [(partner(me, k), partner(h, k)) for k in range(half)]
    block_of = [partner(h // direct, b) for b in range(half // direct)]

    def piece(j):
        begin, size = pieces[j]
        return slice(begin, begin + size)

    def columns(m, j):
        begin, size = pieces[j]
        return pl.ds(pl.multiple_of(m * part + begin, 128), size)

    def fine(j):
        size = part // len(parts)
        return slice(j * size, (j + 1) * size)

    def send(source, target, sent, arrived, device):
        pltpu.make_async_remote_copy(
            src_ref=source,
            dst_ref=target,
            send_sem=sent,
            recv_sem=arrived,
            device_id=device,
            device_id_type=MESH,
        ).start()

    def drain(block, sem):
        pltpu.make_async_copy(block, block, sem).wait()

    def some(j, number):
        return rows_in.at[0, pl.ds(0, number * cap), slice(None) if j is None else piece(j)]

    def many(j, number):
        return rows_in.at[:, pl.ds(0, number * cap), slice(None) if j is None else piece(j)]

    begin = pl.multiple_of(tile * part, part)
    sources = [(all_routes, routes), (all_gates, gates)]
    sources += [
        (all_tokens.at[:, m * part : (m + 1) * part], tokens.at[m]) for m in range(tiles)
    ]
    sources += [
        (all_cache, cache),
        (w_gate, gate_w),
        (w_up, up_w),
        (w_down, down_w),
        (all_time, w_time),
        (all_time_bias, bias_time),
        (all_space, w_space),
        (all_space_bias, bias_space),
        (all_proj.at[pl.ds(begin, part), :], w_proj),
        (all_gain.at[:, pl.ds(begin, part)], gain),
    ]
    loads = [
        pltpu.make_async_copy(source, held, load_sem.at[i])
        for i, (source, held) in enumerate(sources)
    ]
    for load in loads:
        load.start()
    token_loads, loads = loads[: 2 + tiles], loads[2 + tiles :]

    barrier = pltpu.get_barrier_semaphore()
    for k in range(1, half + 1):
        pl.semaphore_signal(barrier, inc=1, device_id=(partner(me, k), tile), device_id_type=MESH)
    for m in range(1, tiles):
        pl.semaphore_signal(
            barrier, inc=1, device_id=(me, (tile + m) % tiles), device_id_type=MESH
        )

    token_loads[0].wait()
    token_loads[1].wait()
    expert = lax.broadcasted_iota(jnp.int32, (sessions, count), 0)
    named = [(routes[k : k + 1, :] == expert).astype(jnp.float32) for k in range(TOPK)]
    earlier = lax.broadcasted_iota(jnp.int32, (count, count), 0) < lax.broadcasted_iota(
        jnp.int32, (count, count), 1
    )
    before = jnp.dot(
        sum(named).astype(jnp.bfloat16),
        earlier.astype(jnp.float32).astype(jnp.bfloat16),
        preferred_element_type=jnp.float32,
    )
    targets = []
    for k in range(TOPK):
        place = jnp.sum(before * named[k], axis=0, keepdims=True).astype(jnp.int32)
        targets.append(routes[k : k + 1, :] * cap + place)
        before = before + named[k]
    weights = []
    for base, hot in ((upper * span, near_hot), ((1 - upper) * span, far_hot)):
        slot = base + lax.broadcasted_iota(jnp.int32, (span, count), 0)
        onehot = jnp.zeros((span, count), jnp.float32)
        weight = jnp.zeros((span, count), jnp.float32)
        for k in range(TOPK):
            hit = slot == targets[k]
            onehot = onehot + jnp.where(hit, 1.0, 0.0)
            weight = weight + jnp.where(hit, gates[k : k + 1, :], 0.0)
        hot[...] = onehot.astype(jnp.bfloat16)
        weights.append(weight)
    for weight, mix in zip(weights, (near_mix, far_mix)):
        weight = weight.T
        high = weight.astype(jnp.bfloat16)
        mix[0] = high
        mix[1] = (weight - high.astype(jnp.float32)).astype(jnp.bfloat16)
    for load in token_loads[2:]:
        load.wait()
    for j in turns:
        for m in range(tiles):
            near_out[m, :, piece(j)] = jnp.dot(
                near_hot[...], tokens[m, :, piece(j)], preferred_element_type=jnp.float32
            ).astype(jnp.bfloat16)
    rows_in[:, rows(h), :] = near_out[:, rows(h), :]
    loads[0].wait()
    newest = head[0]
    slots = [cache[i] for i in range(3)]
    for t, shift in ((1, 0), (0, 2)):
        which = lax.rem(newest + shift, 3)
        past[t] = jnp.where(which == 0, slots[0], jnp.where(which == 1, slots[1], slots[2]))
    pl.semaphore_wait(barrier, half + tiles - 1)

    def hand_over(j):
        here = piece(j)
        send(
            tokens.at[tile, :, here],
            relay_in.at[:, here],
            token_sem.at[n],
            token_sem.at[j],
            (far, tile),
        )

    send(far_hot, hot_in, table_sem.at[0, 0], table_sem.at[1, 0], (far, tile))
    for j in turns:
        here = piece(j)
        for k in range(half - 1, 0, -1):
            other, index = peers[k]
            if k < direct:
                source, target = near_out.at[:, rows(index), here], rows_in.at[:, rows(h), here]
                sems = direct_sem
            else:
                source = near_out.at[tile, rows(index), here]
                target = rows_in.at[tile, rows(h), here]
                sems = near_sem
            send(source, target, sems.at[n], sems.at[j], (other, tile))
    for j in turns:
        hand_over(j)
    send(far_mix, mix_in, table_sem.at[0, 1], table_sem.at[1, 1], (far, tile))

    height = past.shape[1]
    for side, start, step in ((0, height - HALO, 1), (1, 0, tiles - 1)):
        send(
            past.at[:, start : start + HALO],
            halo.at[side],
            halo_sem.at[0, side],
            halo_sem.at[1, side],
            (me, (tile + step) % tiles),
        )

    def forward(block, sems, j):
        for m in range(1, tiles):
            send(block, block, sems.at[m, n], sems.at[m, j], (me, (tile + m) % tiles))

    def near_forward(j):
        drain(some(j, half - direct), near_sem.at[j])
        size = direct * cap
        for b in range(1, half // direct):
            begin = pl.multiple_of(block_of[b] * size, size)
            forward(rows_in.at[tile, pl.ds(begin, size), piece(j)], near_cross, j)

    def relay(j):
        here = piece(j)
        if j == 0:
            drain(hot_in, table_sem.at[1, 0])
        drain(relay_in.at[:, here], token_sem.at[j])
        relay_out[:, here] = jnp.dot(
            hot_in[...], relay_in[:, here], preferred_element_type=jnp.float32
        ).astype(jnp.bfloat16)
        for k in range(half - 1, 0, -1):
            other, index = peers[k]
            send(
                relay_out.at[rows(index), here],
                rows_in.at[tile, rows(h, span), here],
                far_sem.at[n],
                far_sem.at[j],
                (other, tile),
            )
        rows_in[tile, rows(h, span), here] = relay_out[rows(h), here]

    def far_forward(j):
        drain(some(j, half - 1), far_sem.at[j])
        forward(rows_in.at[tile, span : 2 * span, piece(j)], far_cross, j)

    def consume(group, j):
        base = group * span
        if group == 0:
            drain(many(j, direct - 1), direct_sem.at[j])
        for m in range(1, tiles):
            if group == 0:
                drain(some(j, half - direct), near_cross.at[m, j])
            else:
                drain(some(j, half), far_cross.at[m, j])
        if j == 0:
            gate[...] = jnp.zeros_like(gate)
            upward[...] = jnp.zeros_like(upward)

        for m in range(tiles):
            block = rows_in[m, base : base + span, piece(j)]
            gate[...] += across(block, gate_w[:, columns(m, j)])
            upward[...] += across(block, up_w[:, columns(m, j)])

    def activate(group):
        hidden[group] = (silu(gate[...]) * upward[...]).astype(jnp.bfloat16)

    def project(group, m, here):
        span_in = pl.ds(pl.multiple_of(m * part + here.start, 128), here.stop - here.start)
        return jnp.dot(hidden[group], down_w[:, span_in], preferred_element_type=jnp.float32)

    def near_return(j):
        here = piece(j)

        for m in range(tiles):
            near_answer[m, :, here] = project(0, m, here).astype(jnp.bfloat16)

        for k in range(half - 1, 0, -1):
            other, index = peers[k]
            send(
                near_answer.at[:, rows(index), here],
                near_back.at[:, rows(h), here],
                back_sem.at[n],
                back_sem.at[j],
                (other, tile),
            )
        near_back[:, rows(h), here] = near_answer[:, rows(h), here]

    def blend(mix, block):
        return jnp.dot(mix[0], block, preferred_element_type=jnp.float32) + jnp.dot(
            mix[1], block, preferred_element_type=jnp.float32
        )

    def near_blend(j):
        here = piece(j)
        drain(many(j, half - 1), back_sem.at[j])
        for m in range(1, tiles):
            to = (tile + m) % tiles
            near_mixed[m - 1, :, here] = blend(near_mix, near_back[to, :, here]).astype(
                jnp.bfloat16
            )
            send(
                near_mixed.at[m - 1, :, here],
                mixed_in.at[m - 1, :, here],
                mixed_sem.at[m, n],
                mixed_sem.at[m, j],
                (me, to),
            )
        own_mixed[:, here] = blend(near_mix, near_back[tile, :, here])

    def far_answer(j):
        here = fine(j)
        for m in range(1, tiles):
            to = (tile + m) % tiles
            answer[m - 1, :, here] = project(1, to, here).astype(jnp.bfloat16)
            send(
                answer.at[m - 1, :, here],
                stage.at[m - 1, :, here],
                answer_sem.at[m, n * split],
                answer_sem.at[m, j],
                (me, to),
            )

    def far_return(j):
        here = fine(j)
        total = project(1, tile, here)
        for m in range(1, tiles):
            drain(stage.at[m - 1, :, here], answer_sem.at[m, j])
            total = total + stage[m - 1, :, here].astype(jnp.float32)
        reduced[:, here] = total.astype(jnp.bfloat16)
        for k in range(half - 1, 0, -1):
            other, index = peers[k]
            send(
                reduced.at[rows(index), here],
                back.at[rows(h), here],
                other_sem.at[n * split],
                other_sem.at[j],
                (other, tile),
            )
        back[rows(h), here] = reduced[rows(h), here]

    def far_blend(j):
        here = fine(j)
        if j == 0:
            drain(mix_in, table_sem.at[1, 1])
        drain(rows_in.at[0, pl.ds(0, (half - 1) * cap), here], other_sem.at[j])
        partial[:, here] = blend(mix_in, back[:, here]).astype(jnp.bfloat16)
        send(partial.at[:, here], summed.at[:, here], sum_sem.at[n * split], sum_sem.at[j], (far, tile))

    def features(j):
        here = fine(j)
        mixed = own_mixed[:, here]
        for m in range(1, tiles):
            if j % split == 0:
                whole = piece(j // split)
                drain(mixed_in.at[m - 1, :, whole], mixed_sem.at[m, j // split])
            mixed = mixed + mixed_in[m - 1, :, here].astype(jnp.float32)
        drain(summed.at[:, here], sum_sem.at[j])
        mixed = mixed + summed[:, here].astype(jnp.float32)
        feat = (tokens[tile, :, here].astype(jnp.float32) + mixed).astype(jnp.bfloat16)
        feat = feat.astype(jnp.float32)
        scaled = (feat * gain[:, here]).astype(jnp.bfloat16)
        return (
            jnp.sum(feat * feat, axis=1, keepdims=True),
            jnp.dot(scaled, w_proj[here, :], preferred_element_type=jnp.float32),
        )

    tall = frames.shape[1]
    breadth = 2 * GRID_W
    edge = HALO * breadth
    pixels = out.shape[0]
    extended = pixels + 2 * breadth
    grid_rows = count // GRID_W
    own_rows = grid_rows // tiles

    def chosen(mask):
        return jnp.where(mask, 1.0, 0.0).astype(jnp.bfloat16)

    def moved(matrix, value):
        return jnp.dot(matrix, value, preferred_element_type=jnp.float32).astype(jnp.bfloat16)

    def shifts(size):
        to = lax.broadcasted_iota(jnp.int32, (size, size), 0)
        origin = lax.broadcasted_iota(jnp.int32, (size, size), 1)
        column = to % breadth
        return (
            chosen((origin == to - 1) & (column > 0)),
            chosen((origin == to + 1) & (column < breadth - 1)),
        )

    def widen(t, left, right):
        wide[t, :, :channels] = moved(left, frames[t])
        wide[t, :, channels : 2 * channels] = frames[t]
        wide[t, :, 2 * channels :] = moved(right, frames[t])

    def in_time(t):
        total = jnp.zeros((extended, channels), jnp.float32)
        for dy in range(3):
            total = total + jnp.dot(
                wide[t, dy * breadth : dy * breadth + extended, :],
                w_time[3 * t + dy],
                preferred_element_type=jnp.float32,
            )
        return total

    def earlier_frames():
        for side in range(2):
            drain(halo.at[side], halo_sem.at[1, side])
        left, right = shifts(tall)
        for t in range(2):
            top = halo[0, t].reshape(edge, channels)
            bottom = halo[1, t].reshape(edge, channels)
            frames[t, :edge, :] = jnp.where(tile > 0, top, jnp.zeros_like(top))
            frames[t, edge : edge + pixels, :] = past[t].reshape(pixels, channels)
            frames[t, edge + pixels :, :] = jnp.where(
                tile < tiles - 1, bottom, jnp.zeros_like(bottom)
            )
            widen(t, left, right)
        first[...] = in_time(0) + in_time(1) + bias_time[...]

    def last_frame():
        for r in range(own_rows + 2):
            row = tile * own_rows - 1 + r
            at = jnp.clip(row, 0, grid_rows - 1)
            value = coarse_in[pl.ds(pl.multiple_of(at * GRID_W, GRID_W), GRID_W), :]
            above[r * GRID_W : (r + 1) * GRID_W, :] = jnp.where(
                (row >= 0) & (row < grid_rows), value, jnp.zeros_like(value)
            )
        few = above.shape[0]
        pixel = lax.broadcasted_iota(jnp.int32, (tall, few), 0)
        token = lax.broadcasted_iota(jnp.int32, (tall, few), 1)
        spread = chosen(token == (pixel // (2 * breadth)) * GRID_W + (pixel % breadth) // 2)
        frames[2] = moved(spread, above[...].astype(jnp.bfloat16))
        left, right = shifts(tall)
        widen(2, left, right)
        total = first[...] + in_time(2)
        row = tile * (pixels // breadth) - 1 + lax.broadcasted_iota(
            jnp.int32, (extended, channels), 0
        ) // breadth
        inside = (row >= 0) & (row < tiles * (pixels // breadth))
        active = jnp.where(inside, silu(total), 0.0).astype(jnp.bfloat16)
        left, right = shifts(extended)
        wide_active[:, :channels] = moved(left, active)
        wide_active[:, channels : 2 * channels] = active
        wide_active[:, 2 * channels :] = moved(right, active)
        total = frames[2, edge : edge + pixels, :].astype(jnp.float32) + bias_space[...]
        for dy in range(3):
            total = total + jnp.dot(
                wide_active[dy * breadth : dy * breadth + pixels, :],
                w_space[dy],
                preferred_element_type=jnp.float32,
            )
        out[...] = total.astype(jnp.bfloat16)

    for load in loads[1:3]:
        load.wait()
    for j in turns:
        near_forward(j)
        relay(j)
    for j in turns:
        if j < n - 1:
            far_forward(j)
        consume(0, j)
    activate(0)
    loads[3].wait()
    for j in turns:
        near_return(j)
        if j == 0:
            far_forward(n - 1)
    for load in loads[4:]:
        load.wait()
    for j in turns:
        consume(1, j)
    activate(1)
    for j in parts:
        far_answer(j)
    earlier_frames()
    found = []
    for j in range(len(parts) + 7):
        if j < len(parts):
            far_return(j)
            if j % split == 0:
                near_blend(j // split)
        if 0 <= j - 2 < len(parts):
            far_blend(j - 2)
        if 0 <= j - 7:
            found.append(features(j - 7))
    square = sum(pair[0] for pair in found)
    coarse = sum(pair[1] for pair in found)
    lane = lax.broadcasted_iota(jnp.int32, (count, 128), 1)
    high = square.astype(jnp.bfloat16).astype(jnp.float32)
    mine[:, :channels] = coarse.astype(jnp.bfloat16)
    mine[:, channels:] = jnp.where(
        lane == 0, high, jnp.where(lane == 1, square - high, 0.0)
    ).astype(jnp.bfloat16)
    for m in range(1, tiles):
        send(mine, theirs.at[m - 1], last_sem.at[0, m], last_sem.at[1, m], (me, (tile + m) % tiles))
    for m in range(1, tiles):
        drain(theirs.at[m - 1], last_sem.at[1, m])
        coarse = coarse + theirs[m - 1, :, :channels].astype(jnp.float32)
        square = square + jnp.sum(
            theirs[m - 1, :, channels:].astype(jnp.float32), axis=1, keepdims=True
        )
    coarse_in[...] = coarse * lax.rsqrt(square * (1.0 / width) + epsilon)
    last_frame()

    drain(far_hot, table_sem.at[0, 0])
    drain(far_mix, table_sem.at[0, 1])
    for side in range(2):
        drain(halo.at[side], halo_sem.at[0, side])
    drain(relay_in, token_sem.at[n])
    drain(some(None, half - direct), near_sem.at[n])
    drain(many(None, direct - 1), direct_sem.at[n])
    drain(some(None, half - 1), far_sem.at[n])
    drain(many(None, half - 1), back_sem.at[n])
    drain(some(None, half - 1), other_sem.at[n * split])
    drain(summed, sum_sem.at[n * split])
    for m in range(1, tiles):
        drain(some(None, half - direct), near_cross.at[m, n])
        drain(some(None, half), far_cross.at[m, n])
        drain(mixed_in.at[m - 1], mixed_sem.at[m, n])
        drain(stage.at[m - 1], answer_sem.at[m, n * split])
        drain(theirs.at[m - 1], last_sem.at[0, m])


def layer(
    routes,
    gates,
    head,
    gain,
    tokens,
    w_gate,
    w_up,
    w_down,
    w_proj,
    cache,
    w_time,
    bias_time,
    w_space,
    bias_space,
    sizes,
):
    sessions, tiles, cap = sizes
    count, width = tokens.shape
    hid, part, half = w_gate.shape[0], width // tiles, sessions // 2
    span, channels = half * cap, w_proj.shape[1]
    pixels = cache.shape[1] * cache.shape[2]
    breadth = 2 * GRID_W
    tall = pixels + 2 * HALO * breadth
    few = count // tiles + 2 * GRID_W
    pieces = pieces_of(part)
    hbm = pl.BlockSpec(memory_space=pltpu.HBM)
    low, full = jnp.bfloat16, jnp.float32
    n = len(pieces)
    split = fine_of(part, n)
    held = [
        (routes.shape, routes.dtype),
        (gates.shape, full),
        ((1, part), full),
        ((tiles, count, part), low),
        (w_gate.shape, low),
        (w_up.shape, low),
        (w_down.shape, low),
        ((part, channels), low),
        (cache.shape, low),
        (w_time.shape, low),
        (bias_time.shape, full),
        (w_space.shape, low),
        (bias_space.shape, full),
        ((2,) + cache.shape[1:], low),
        ((2, 2, HALO) + cache.shape[2:], low),
        ((span, count), low),
        ((span, count), low),
        ((2, count, span), low),
        ((2, count, span), low),
        ((span, count), low),
        ((2, count, span), low),
        ((count, part), low),
        ((tiles, span, part), low),
        ((span, part), low),
        ((tiles, 2 * span, part), low),
        ((span, hid), full),
        ((span, hid), full),
        ((2, span, hid), low),
        ((tiles, span, part), low),
        ((tiles, span, part), low),
        ((tiles - 1, count, part), low),
        ((count, part), full),
        ((tiles - 1, count, part), low),
        ((tiles - 1, span, part), low),
        ((tiles - 1, span, part), low),
        ((span, part), low),
        ((span, part), low),
        ((count, part), low),
        ((count, part), low),
        ((count, channels + 128), low),
        ((tiles - 1, count, channels + 128), low),
        ((count, channels), full),
        ((few, channels), full),
        ((3, tall, channels), low),
        ((3, tall, 3 * channels), low),
        ((pixels + 2 * breadth, channels), full),
        ((pixels + 2 * breadth, 3 * channels), low),
    ]
    sems = [
        (12 + tiles,),
        (2, 2),
        (2, 2),
        (n + 1,),
        (n + 1,),
        (n + 1,),
        (n + 1,),
        (tiles, n + 1),
        (tiles, n + 1),
        (n + 1,),
        (tiles, n + 1),
        (tiles, n * split + 1),
        (n * split + 1,),
        (n * split + 1,),
        (2, tiles),
    ]
    return pl.pallas_call(
        functools.partial(layer_kernel, sessions, tiles, cap, pieces),
        out_shape=jax.ShapeDtypeStruct((pixels, channels), low),
        in_specs=[hbm, hbm, pl.BlockSpec(memory_space=pltpu.SMEM)] + [hbm] * 11,
        out_specs=VMEM,
        scratch_shapes=[pltpu.VMEM(*each) for each in held]
        + [pltpu.SemaphoreType.DMA(each) for each in sems],
        compiler_params=pltpu.CompilerParams(
            collective_id=0, has_side_effects=True, vmem_limit_bytes=60 * 2**20
        ),
        name="layer",
    )(
        routes,
        gates,
        head,
        gain,
        tokens,
        w_gate,
        w_up,
        w_down,
        w_proj,
        cache,
        w_time,
        bias_time,
        w_space,
        bias_space,
    )


def body(
    tokens,
    routes,
    gates,
    w_gate,
    w_up,
    w_down,
    feat_gain,
    w_proj,
    conv_time,
    bias_time,
    conv_space,
    bias_space,
    frame_cache,
    cache_head,
):
    sessions, tiles = lax.axis_size("sess"), lax.axis_size("exp")
    channels = w_proj.shape[-1]
    local = tokens[0]
    tok_count = local.shape[0]
    cap = 2 * tok_count * TOPK // sessions
    height, breadth = frame_cache.shape[2:4]
    result = layer(
        routes[0].T,
        gates[0].T,
        cache_head,
        feat_gain[None, :],
        local,
        w_gate[0].T,
        w_up[0].T,
        w_down[0],
        w_proj,
        frame_cache[:, 0],
        conv_time.reshape(9, 3 * channels, channels),
        bias_time[None, :],
        conv_space.reshape(3, 3 * channels, channels),
        bias_space[None, :],
        (sessions, tiles, cap),
    )
    return result.reshape(1, height, breadth, channels)


def solution(mesh):
    return jax.shard_map(
        body,
        mesh=mesh,
        in_specs=(
            P("sess", None, None),
            P("sess", None, None),
            P("sess", None, None),
            P("sess", None, "exp"),
            P("sess", None, "exp"),
            P("sess", "exp", None),
            P(),
            P(),
            P(),
            P(),
            P(),
            P(),
            P(None, "sess", "exp", None, None),
            P("sess"),
        ),
        out_specs=P("sess", "exp", None, None),
        check_vma=False,
    )
```
